256 devices in a mesh: dp: 64 (over x, z, core), tensor: 4 (over y).
Axes of the slice: x: 4, y: 4, z: 8, core: 2. Of those that a mesh axis runs over, the one named last changes fastest.
Arguments:
- activations: bfloat16 [768, 8192], P('dp', 'tensor'), may hold values from -400 to 400, as said below
- weight: bfloat16 [8192, 28672], P('dp', 'tensor'), may hold values from -0.0625 to 0.0625
Outputs:
- channel_mean: float32 [8192], P('dp')
- column_errors: float32 [4, 28672], P(None, ('tensor', 'dp'))
- errors: float32 [4], replicated
The draws below stay inside these ranges and needn't reach their ends.
Inputs may be any that keep to these rules, and one draw needn't show every extreme that they name: activations and weight are finite real values within the ranges stated above.
All inputs are finite; a program needn't handle non-finite values.
Results may differ from the reference program's by a relative error of at most 0.0012.
The reference program's roundings to bfloat16 on the way (of `dequant`) count: a program that leaves them out, or rounds other values in their place, can miss the bound.
Values may be sent and summed in bfloat16 or wider, within the bound.
A program may use at most 128 MiB of HBM per device.

```python
import math
import jax
import jax.numpy as jnp
from jax import lax

D = 8192
F = 28672
GROUP = 128
GRID = 4
TOKENS = 768
N_TENSOR = 4


def draw_activations(key, part):
    base_key = jax.random.fold_in(key, 11)
    key_main, key_row, key_col = jax.random.split(base_key, 3)
    position = jnp.arange(TOKENS, dtype=jnp.float32) / max(TOKENS - 1, 1)
    row_scale = jnp.exp(math.log(4.0) * position + jax.random.uniform(key_row, (TOKENS,), jnp.float32, -0.3, 0.3))
    col_scale = jnp.exp(jax.random.uniform(key_col, (D,), jnp.float32, 0.0, math.log(10.0)))
    values = jnp.clip(jax.random.normal(key_main, (TOKENS, D), jnp.float32), -6.0, 6.0)
    return (values * row_scale[:, None] * col_scale[None, :]).astype(jnp.bfloat16)


def level_of(own_key, shape, cuts, smallest, top_value):
    gain, own = 1.0, jax.random.fold_in(own_key, 6)
    for axis_at, parts in cuts:
        draws = jnp.exp(jax.random.uniform(jax.random.fold_in(own, axis_at), (parts,), jnp.float32, smallest / len(cuts), top_value / len(cuts)))
        gain = gain * jnp.repeat(draws, shape[axis_at] // parts).reshape([-1 if axis == axis_at else 1 for axis in range(len(shape))])
    return gain


def scatter_about(stream_key, extent, spread, limit, cuts=(), kind=jnp.bfloat16):
    entries = spread * jax.random.normal(stream_key, extent, jnp.float32)
    if cuts:
        entries = entries * level_of(stream_key, extent, cuts, -0.22, 0.18)
    return jnp.clip(entries, -limit, limit).astype(kind)


def setup_inputs(seed: int = 0) -> dict:
    splits = jax.random.split(jax.random.key(seed), 3)
    return {
        "activations": draw_activations(jax.random.fold_in(splits[2], 71), 0),
        "weight": scatter_about(splits[1], (D, F), D ** -0.5, 0.0625, ((0, 64), (1, 4))),
    }


def soft_round(values):
    return values - jnp.sin(2.0 * math.pi * values) / (2.0 * math.pi)

def scale_table(channel_mean):
    ratios = jnp.arange(GRID, dtype=jnp.float32) / GRID
    raw = jnp.exp(ratios[:, None] * jnp.log(channel_mean)[None, :])
    top = lax.optimization_barrier(jnp.max(raw, axis=1, keepdims=True))
    bottom = lax.optimization_barrier(jnp.min(raw, axis=1, keepdims=True))
    return raw / jnp.sqrt(top * bottom)

def block_errors(activations, block, scales):
    base_out = jnp.dot(activations, block, preferred_element_type=jnp.float32)
    width = block.shape[1]
    weight_float = block.astype(jnp.float32)

    def one_ratio(factor):
        scaled = weight_float * factor[:, None]
        grouped = scaled.reshape(D // GROUP, GROUP, width)
        quant_step = (lax.optimization_barrier(jnp.max(jnp.abs(grouped), axis=1, keepdims=True)) + 1e-06) / 7.0
        levels = soft_round(grouped / quant_step)
        dequant = ((levels * quant_step).reshape(D, width) / factor[:, None]).astype(jnp.bfloat16)
        quant_out = jnp.dot(activations, dequant, preferred_element_type=jnp.float32)
        residue = quant_out - base_out
        return lax.optimization_barrier(jnp.sum(residue * residue, axis=0))
    return lax.map(one_ratio, scales)

def reference(activations, weight):
    act_float = activations.astype(jnp.float32)
    channel_mean = lax.optimization_barrier(jnp.mean(jnp.abs(act_float), axis=0)) + 1e-06
    scales = scale_table(channel_mean)
    blocks = jnp.transpose(weight.reshape(D, N_TENSOR, F // N_TENSOR), (1, 0, 2))
    column_sums = lax.map(lambda block: block_errors(activations, block, scales), blocks)
    column_sums = jnp.transpose(column_sums, (1, 0, 2)).reshape(GRID, F)
    column_errors = column_sums / TOKENS
    errors = lax.optimization_barrier(jnp.sum(column_sums, axis=1)) / (TOKENS * F)
    return (channel_mean, column_errors, errors)
```

```python
import functools

import jax
import jax.numpy as jnp
from jax import lax
from jax.experimental import pallas as pl
from jax.experimental.pallas import tpu as pltpu
from jax.sharding import Mesh
from jax.sharding import PartitionSpec as P

D = 8192
F = 28672
GROUP = 128
GRID = 4
TOKENS = 768
NX, NZ, NC, NY = 4, 8, 2, 4
PLANE = NX * NZ
ACTIVE = 28
ROWS = 24
HALF = 1024
WIDE = 256
SUB = HALF // GROUP
DP = ("x", "z", "c")
Z_ORDER = (0, -1, 1, -2, 2, -3, 3, -4)
WAVE = (6.579736255173805, -12.987875283620534, 12.207951996649596, -6.691021837978725, 2.380346767313312, -0.5278301996489366)
MESH_ID = pl.DeviceIdType.MESH


def kernel(
    act, w, mean_out, cols_out, errors_out,
    swap, abuf, dbuf, acc, part, other, stat, staty, ends, table, inverse, tiles, mine, finals, finaly, finalc,
    send_small, send_piece, send_w, send_part,
    swap_sem, z_sem, xl_sem, xr_sem, x2_sem, yd_sem, yu_sem, y2_sem, w_sem, stat_sem, staty_sem, ends_sem,
    part_sem, tile_sem, fin_sem, finy_sem, finc_sem, own_sem,
):
    x, z, c, y = (lax.axis_index(name) for name in ("x", "z", "c", "y"))
    me = x * NZ + z
    active = me < ACTIVE

    def device(dx=0, dz=0, dc=0, dy=0):
        return {
            "x": lax.rem(x + dx + NX, NX),
            "z": lax.rem(z + dz + NZ, NZ),
            "c": lax.rem(c + dc, NC),
            "y": lax.rem(y + dy + NY, NY),
        }

    def remote(src, dst, send, recv, to):
        return pltpu.make_async_remote_copy(
            src_ref=src, dst_ref=dst, send_sem=send, recv_sem=recv, device_id=to, device_id_type=MESH_ID
        )

    def arrived(ref, sem):
        pltpu.make_async_copy(ref, ref, sem).wait()

    barrier = pltpu.get_barrier_semaphore()

    def greet(n, _):
        to = device(n // (NZ * NC), lax.rem(n // NC, NZ), lax.rem(n, NC))
        pl.semaphore_signal(barrier, inc=1, device_id=to, device_id_type=MESH_ID)
        return 0

    lax.fori_loop(1, PLANE * NC, greet, 0)
    for dy in range(1, NY):
        pl.semaphore_signal(barrier, inc=1, device_id=device(dy=dy), device_id_type=MESH_ID)
    pl.semaphore_wait(barrier, PLANE * NC - 1 + NY - 1)

    def lanes(group):
        return pl.ds(pl.multiple_of(group * GROUP, GROUP), GROUP)

    for j in range(SUB):
        remote(
            act.at[:, lanes(2 * j + 1 - c)], swap.at[j], send_small.at[0], swap_sem.at[j], device(dc=1)
        ).start()
    here = c == 0
    for j in range(SUB):
        arrived(swap.at[j], swap_sem.at[j])
        own = act[:, lanes(2 * j + c)].astype(jnp.float32)
        peer = swap[j].astype(jnp.float32)
        block = jnp.concatenate([jnp.where(here, own, peer), jnp.where(here, peer, own)], axis=0)
        stat[me, j : j + 1, :] = jnp.sum(jnp.abs(block), axis=0, keepdims=True)
        abuf[y, me, :, j * GROUP : (j + 1) * GROUP] = block.astype(jnp.bfloat16)

    def send_stat(n, _):
        to = device(n // NZ, lax.rem(n, NZ))
        remote(stat.at[me], stat.at[me], send_small.at[1], stat_sem.at[me], to).start()
        return 0

    lax.fori_loop(1, PLANE, send_stat, 0)

    def send_weight(dx, dz):
        to = device(dx, dz)
        there = to["x"] * NZ + to["z"]

        @pl.when(there < ACTIVE)
        def _():
            columns = w.at[:, pl.ds(pl.multiple_of(there * WIDE, WIDE), WIDE)]
            if dx == 0 and dz == 0:
                pltpu.make_async_copy(columns, dbuf.at[GRID, me], own_sem.at[0]).start()
            else:
                remote(columns, dbuf.at[GRID, me], send_w.at[0], w_sem.at[me], to).start()

    def along(index):
        return lax.rem(z + index + NZ, NZ)

    def piece(yy, xx, k):
        return abuf.at[lax.rem(yy + NY, NY), lax.rem(xx + NX, NX) * NZ + along(Z_ORDER[k])]

    def pass_on(ref, sem, **to):
        remote(ref, ref, send_piece.at[0], sem, device(**to)).start()

    def up_and_down(ref, n):
        pass_on(ref, yd_sem.at[n], dy=1)
        pass_on(ref, yu_sem.at[n], dy=-1)

    for k in range(NZ):
        ref = piece(y, x, k)
        if k > 0:
            arrived(ref, z_sem.at[k])
        if k == 0 or (k % 2 == 1 and k < 7):
            pass_on(ref, z_sem.at[k + 1 if k == 0 else k + 2], dz=1)
        if k == 0 or (k % 2 == 0 and k < 6):
            pass_on(ref, z_sem.at[k + 2], dz=-1)
        pass_on(ref, xl_sem.at[k], dx=1)
        pass_on(ref, xr_sem.at[k], dx=-1)
        up_and_down(ref, k)
        for dx in (2, 1, 3, 0):
            send_weight(dx, Z_ORDER[7 - k])

    def hear_stat(n, _):
        there = lax.rem(x + n // NZ, NX) * NZ + lax.rem(z + lax.rem(n, NZ), NZ)
        arrived(stat.at[there], stat_sem.at[there])
        return 0

    lax.fori_loop(1, PLANE, hear_stat, 0)
    staty[y] = jnp.sum(stat[...], axis=0)
    for dy in range(1, NY):
        remote(staty.at[y], staty.at[y], send_small.at[1], staty_sem.at[y], device(dy=dy)).start()

    for k in range(NZ):
        left, right = piece(y, x - 1, k), piece(y, x + 1, k)
        arrived(left, xl_sem.at[k])
        if k < 4:
            pass_on(left, x2_sem.at[k], dx=1)
        up_and_down(left, 8 + 2 * k)
        arrived(right, xr_sem.at[k])
        if k >= 4:
            pass_on(right, x2_sem.at[k], dx=-1)
        up_and_down(right, 9 + 2 * k)

    for dy in range(1, NY):
        there = lax.rem(y + dy, NY)
        arrived(staty.at[there], staty_sem.at[there])
    channel_mean = staty[...].reshape(PLANE, GROUP) / TOKENS + 1e-06
    own_mean = staty[x, pl.ds(z, 1), :] / TOKENS + 1e-06
    mean_out[...] = own_mean
    log_mean = jnp.log(channel_mean)
    ends[c, 0] = jnp.broadcast_to(jnp.max(log_mean, axis=0, keepdims=True), (8, GROUP))
    ends[c, 1] = jnp.broadcast_to(jnp.min(log_mean, axis=0, keepdims=True), (8, GROUP))
    remote(ends.at[c], ends.at[c], send_small.at[2], ends_sem.at[0], device(dc=1)).start()
    for k in range(NZ):
        far = piece(y, x + 2, k)
        arrived(far, x2_sem.at[k])
        up_and_down(far, 24 + k)
    arrived(ends.at[1 - c], ends_sem.at[0])
    top = jnp.max(jnp.maximum(ends[0, 0], ends[1, 0]), axis=(0, 1), keepdims=True)
    bottom = jnp.min(jnp.minimum(ends[0, 1], ends[1, 1]), axis=(0, 1), keepdims=True)
    rows = []
    for k in range(1, GRID):
        ratio = k / GRID
        level = jnp.sqrt(jnp.exp(ratio * top) * jnp.exp(ratio * bottom))
        rows.append(jnp.exp(ratio * log_mean) / level)
    rows.append(jnp.ones((PLANE, GROUP), jnp.float32))
    stacked = jnp.concatenate(rows, axis=0)
    table[...] = stacked.T
    inverse[...] = (1.0 / stacked).T

    def quantize(slot):
        weight = dbuf[GRID, slot].astype(jnp.float32)
        factors = pltpu.roll(table[...], GROUP - slot, 1)
        backs = pltpu.roll(inverse[...], GROUP - slot, 1)
        for k in range(GRID):
            if k == 0:
                scaled = weight
            else:
                at = (k - 1) * PLANE
                scaled = weight * factors[:, at : at + 1]
            step = (jnp.max(jnp.abs(scaled), axis=0, keepdims=True) + 1e-06) * (1.0 / 7.0)
            value = scaled * (1.0 / step)
            whole = jnp.round(value)
            rest = value - whole
            square = rest * rest
            wave = jnp.full_like(square, WAVE[-1])
            for term in WAVE[-2::-1]:
                wave = wave * square + term
            level = whole + rest * square * wave
            result = level * step
            if k > 0:
                result = result * backs[:, at : at + 1]
            dbuf[k, slot] = result.astype(jnp.bfloat16)

    def relay(n, _):
        xx, zz = x, z
        order = jnp.where(n < 8, n, jnp.where(n < 24, (n - 8) // 2, n - 24))
        dx = jnp.where(n < 8, 0, jnp.where(n < 24, jnp.where(lax.rem(n, 2) == 0, -1, 1), 2))
        dz = jnp.where(lax.rem(order, 2) == 1, -((order + 1) // 2), order // 2)
        slot = lax.rem(xx + dx + NX, NX) * NZ + lax.rem(zz + dz + NZ, NZ)
        below = abuf.at[lax.rem(y + NY - 1, NY), slot]
        above = abuf.at[lax.rem(y + 1, NY), slot]
        arrived(below, yd_sem.at[n])

        @pl.when(lax.rem(n, 2) == 0)
        def _():
            pass_on(below, y2_sem.at[n], dy=1)

        arrived(above, yu_sem.at[n])

        @pl.when(lax.rem(n, 2) == 1)
        def _():
            pass_on(above, y2_sem.at[n], dy=-1)

        @pl.when(active)
        def _():
            @pl.when(slot == me)
            def _():
                pltpu.make_async_copy(dbuf.at[GRID, slot], dbuf.at[GRID, slot], own_sem.at[0]).wait()

            @pl.when(slot != me)
            def _():
                arrived(dbuf.at[GRID, slot], w_sem.at[slot])

            quantize(slot)

        return 0

    lax.fori_loop(0, PLANE, relay, 0)

    def last(n, _):
        order = jnp.where(n < 8, n, jnp.where(n < 24, (n - 8) // 2, n - 24))
        dx = jnp.where(n < 8, 0, jnp.where(n < 24, jnp.where(lax.rem(n, 2) == 0, -1, 1), 2))
        dz = jnp.where(lax.rem(order, 2) == 1, -((order + 1) // 2), order // 2)
        slot = lax.rem(x + dx + NX, NX) * NZ + lax.rem(z + dz + NZ, NZ)
        arrived(abuf.at[lax.rem(y + 2, NY), slot], y2_sem.at[n])
        return 0

    lax.fori_loop(0, PLANE, last, 0)

    @pl.when(active)
    def _():
        def multiply(n, _):
            block, k = n // (GRID + 1), lax.rem(n, GRID + 1)
            lhs = abuf[block].reshape(TOKENS, HALF)
            rhs = dbuf[k, pl.ds(block * SUB, SUB)].reshape(HALF, WIDE)
            product = jnp.dot(lhs, rhs, preferred_element_type=jnp.float32)

            @pl.when(block == 0)
            def _():
                acc[k] = product

            @pl.when(block > 0)
            def _():
                acc[k] += product

            return 0

        lax.fori_loop(0, NY * (GRID + 1), multiply, 0)
        for k in range(GRID):
            residue = acc[k] - acc[GRID]
            part[k, 0] = residue[:, :GROUP]
            part[k, 1] = residue[:, GROUP:]
            remote(part.at[k, 1 - c], other.at[k], send_part.at[0], part_sem.at[k], device(dc=1)).start()
        sums = []
        for k in range(GRID):
            arrived(other.at[k], part_sem.at[k])
            residue = part[k, c] + other[k]
            sums.append(jnp.sum(residue * residue, axis=0, keepdims=True))
        mine[...] = jnp.concatenate(sums + [jnp.zeros((GRID, GROUP), jnp.float32)], axis=0)

    @pl.when(jnp.logical_not(active))
    def _():
        mine[...] = jnp.zeros((8, GROUP), jnp.float32)

    tile = 2 * me + c
    owner = (tile // 7) * 8 + lax.rem(tile, 7)

    def send_tile(to_index, slot):
        to = {"x": to_index // (NZ * NC), "z": lax.rem(to_index // NC, NZ), "c": lax.rem(to_index, NC), "y": y}
        same = to_index == tile

        @pl.when(jnp.logical_not(same))
        def _():
            remote(mine, tiles.at[slot], send_small.at[3], tile_sem.at[slot], to).start()

        @pl.when(same)
        def _():
            tiles[slot] = mine[...]

    @pl.when(active)
    def _():
        send_tile(owner, 1)
        send_tile(owner + 1, 0)

    finals[me] = mine[...]

    def send_final(n, _):
        remote(finals.at[me], finals.at[me], send_small.at[4], fin_sem.at[me], device(n // NZ, lax.rem(n, NZ))).start()
        return 0

    lax.fori_loop(1, PLANE, send_final, 0)

    place = lax.rem(tile, 8)
    before = (tile // 8) * 7 + place - 1
    after = before + 1

    @pl.when(jnp.logical_and(place > 0, before != tile))
    def _():
        arrived(tiles.at[0], tile_sem.at[0])

    @pl.when(place == 0)
    def _():
        tiles[0] = jnp.zeros((8, GROUP), jnp.float32)

    @pl.when(jnp.logical_and(place < 7, after != tile))
    def _():
        arrived(tiles.at[1], tile_sem.at[1])

    @pl.when(place == 7)
    def _():
        tiles[1] = jnp.zeros((8, GROUP), jnp.float32)

    shift = 16 * place
    lane = lax.broadcasted_iota(jnp.int32, (8, GROUP), 1)
    joined = jnp.where(lane < shift, pltpu.roll(tiles[0], shift, 1), pltpu.roll(tiles[1], shift, 1))
    cols_out[...] = joined / TOKENS

    def hear_final(n, _):
        there = lax.rem(x + n // NZ, NX) * NZ + lax.rem(z + lax.rem(n, NZ), NZ)
        arrived(finals.at[there], fin_sem.at[there])
        return 0

    lax.fori_loop(1, PLANE, hear_final, 0)
    finaly[y] = jnp.sum(finals[...], axis=0)
    for dy in range(1, NY):
        remote(finaly.at[y], finaly.at[y], send_small.at[4], finy_sem.at[y], device(dy=dy)).start()
    for dy in range(1, NY):
        there = lax.rem(y + dy, NY)
        arrived(finaly.at[there], finy_sem.at[there])
    finalc[c] = jnp.sum(finaly[...], axis=0)
    remote(finalc.at[c], finalc.at[c], send_small.at[4], finc_sem.at[0], device(dc=1)).start()
    arrived(finalc.at[1 - c], finc_sem.at[0])
    total = jnp.sum(finalc[0] + finalc[1], axis=1, keepdims=True)
    errors_out[...] = jnp.broadcast_to(total / (TOKENS * F), (8, GROUP))

    for j in range(SUB):
        arrived(swap.at[j], send_small.at[0])

    def left_stat(n, _):
        arrived(stat.at[0], send_small.at[1])
        return 0

    lax.fori_loop(0, PLANE - 1 + NY - 1, left_stat, 0)
    arrived(ends.at[0], send_small.at[2])

    @pl.when(active)
    def _():
        @pl.when(owner != tile)
        def _():
            arrived(mine, send_small.at[3])

        @pl.when(owner + 1 != tile)
        def _():
            arrived(mine, send_small.at[3])

        for k in range(GRID):
            arrived(other.at[0], send_part.at[0])

    def left_final(n, _):
        arrived(finals.at[0], send_small.at[4])
        return 0

    lax.fori_loop(0, PLANE - 1 + NY - 1 + 1, left_final, 0)

    def left_piece(n, _):
        arrived(abuf.at[0, 0], send_piece.at[0])
        return 0

    lax.fori_loop(0, NZ - 1 + 2 * NZ + NZ + 2 * PLANE + PLANE, left_piece, 0)

    def left_weight(n, _):
        arrived(dbuf.at[GRID, 0], send_w.at[0])
        return 0

    lax.fori_loop(0, jnp.where(active, ACTIVE - 1, ACTIVE), left_weight, 0)


def on_device(activations, weight):
    vmem = pl.BlockSpec(memory_space=pltpu.VMEM)
    dma = pltpu.SemaphoreType.DMA
    f32, bf16 = jnp.float32, jnp.bfloat16
    own_mean, cols, errors = pl.pallas_call(
        kernel,
        out_shape=(
            jax.ShapeDtypeStruct((1, GROUP), f32),
            jax.ShapeDtypeStruct((8, GROUP), f32),
            jax.ShapeDtypeStruct((8, GROUP), f32),
        ),
        in_specs=[vmem, pl.BlockSpec(memory_space=pl.ANY)],
        out_specs=(vmem, vmem, vmem),
        scratch_shapes=[
            pltpu.VMEM((SUB, ROWS // 2, GROUP), bf16),
            pltpu.VMEM((NY, PLANE, ROWS, HALF), bf16),
            pltpu.VMEM((GRID + 1, PLANE, GROUP, WIDE), bf16),
            pltpu.VMEM((GRID + 1, TOKENS, WIDE), f32),
            pltpu.VMEM((GRID, NC, TOKENS, GROUP), f32),
            pltpu.VMEM((GRID, TOKENS, GROUP), f32),
            pltpu.VMEM((PLANE, 8, GROUP), f32),
            pltpu.VMEM((NY, 8, GROUP), f32),
            pltpu.VMEM((NC, 2, 8, GROUP), f32),
            pltpu.VMEM((GROUP, GROUP), f32),
            pltpu.VMEM((GROUP, GROUP), f32),
            pltpu.VMEM((2, 8, GROUP), f32),
            pltpu.VMEM((8, GROUP), f32),
            pltpu.VMEM((PLANE, 8, GROUP), f32),
            pltpu.VMEM((NY, 8, GROUP), f32),
            pltpu.VMEM((NC, 8, GROUP), f32),
            dma((5,)),
            dma((1,)),
            dma((1,)),
            dma((1,)),
            dma((SUB,)),
            dma((NZ,)),
            dma((NZ,)),
            dma((NZ,)),
            dma((NZ,)),
            dma((PLANE,)),
            dma((PLANE,)),
            dma((PLANE,)),
            dma((PLANE,)),
            dma((PLANE,)),
            dma((NY,)),
            dma((1,)),
            dma((GRID,)),
            dma((2,)),
            dma((PLANE,)),
            dma((NY,)),
            dma((1,)),
            dma((1,)),
        ],
        compiler_params=pltpu.CompilerParams(
            collective_id=0, has_side_effects=True, vmem_limit_bytes=60 * 1024 * 1024
        ),
    )(activations, weight)
    return own_mean[0], cols[:GRID, :112], errors[:GRID, 0]


def solution(mesh):
    torus = Mesh(mesh.devices.reshape(NX, NZ, NC, NY), ("x", "z", "c", "y"))
    placed = (P(DP, "y"), P(DP, "y"))
    return jax.shard_map(
        on_device,
        mesh=torus,
        in_specs=placed,
        out_specs=(P(DP), P(None, ("y", "x", "z", "c")), P()),
        check_vma=False,
    )
```

```python
import functools

import jax
import jax.numpy as jnp
from jax import lax
from jax.experimental import pallas as pl
from jax.experimental.pallas import tpu as pltpu
from jax.sharding import Mesh
from jax.sharding import PartitionSpec as P

D = 8192
F = 28672
GROUP = 128
GRID = 4
TOKENS = 768
NX, NZ, NC, NY = 4, 8, 2, 4
PLANE = NX * NZ
ACTIVE = 28
ROWS = 24
HALF = 1024
WIDE = 256
SUB = HALF // GROUP
DP = ("x", "z", "c")
Z_ORDER = (0, -1, 1, -2, 2, -3, 3, -4)
X_ORDER = (0, 3, 1, 2)
WAVE = (6.579736255173805, -12.987875283620534, 12.207951996649596, -6.691021837978725, 2.380346767313312, -0.5278301996489366)
EARLY = (
    (),
    ((0, -4),),
    ((0, 3),),
    ((0, -3),),
    (),
    ((0, 2),),
    ((0, -2),),
    ((0, 1), (0, -1), (0, 0)),
)
MESH_ID = pl.DeviceIdType.MESH


def kernel(
    act, w, mean_out, cols_out, errors_out,
    swap, abuf, dbuf, acc, part, other, stat, staty, ends, table, inverse, tiles, mine, finals, finaly,
    send_small, send_piece, send_w, send_part,
    swap_sem, z_sem, xl_sem, xr_sem, x2_sem, yd_sem, yu_sem, y2_sem, w_sem, stat_sem, staty_sem, ends_sem,
    part_sem, tile_sem, fin_sem, finy_sem, own_sem,
):
    x, z, c, y = (lax.axis_index(name) for name in ("x", "z", "c", "y"))
    me = x * NZ + z
    active = me < ACTIVE

    def device(dx=0, dz=0, dc=0, dy=0):
        return {
            "x": lax.rem(x + dx + NX, NX),
            "z": lax.rem(z + dz + NZ, NZ),
            "c": lax.rem(c + dc, NC),
            "y": lax.rem(y + dy + NY, NY),
        }

    def remote(src, dst, send, recv, to):
        return pltpu.make_async_remote_copy(
            src_ref=src, dst_ref=dst, send_sem=send, recv_sem=recv, device_id=to, device_id_type=MESH_ID
        )

    def arrived(ref, sem):
        pltpu.make_async_copy(ref, ref, sem).wait()

    barrier = pltpu.get_barrier_semaphore()

    def greet(n, _):
        to = device(n // (NZ * NC), lax.rem(n // NC, NZ), lax.rem(n, NC))
        pl.semaphore_signal(barrier, inc=1, device_id=to, device_id_type=MESH_ID)
        return 0

    lax.fori_loop(1, PLANE * NC, greet, 0)
    for dy in range(1, NY):
        for dc in range(NC):
            pl.semaphore_signal(barrier, inc=1, device_id=device(dy=dy, dc=dc), device_id_type=MESH_ID)
    for k in range(GRID + 1):
        acc[k] = jnp.zeros((TOKENS, WIDE), jnp.float32)
    pl.semaphore_wait(barrier, PLANE * NC - 1 + (NY - 1) * NC)

    def lanes(group):
        return pl.ds(pl.multiple_of(group * GROUP, GROUP), GROUP)

    for j in range(SUB):
        remote(
            act.at[:, lanes(2 * j + 1 - c)], swap.at[j], send_small.at[0], swap_sem.at[j], device(dc=1)
        ).start()
    here = c == 0
    for j in range(SUB):
        arrived(swap.at[j], swap_sem.at[j])
        own = act[:, lanes(2 * j + c)].astype(jnp.float32)
        peer = swap[j].astype(jnp.float32)
        block = jnp.concatenate([jnp.where(here, own, peer), jnp.where(here, peer, own)], axis=0)
        stat[me, j : j + 1, :] = jnp.sum(jnp.abs(block), axis=0, keepdims=True)
        abuf[y, me, :, j * GROUP : (j + 1) * GROUP] = block.astype(jnp.bfloat16)

    def send_stat(n, _):
        to = device(n // NZ, lax.rem(n, NZ))
        remote(stat.at[me], stat.at[me], send_small.at[1], stat_sem.at[me], to).start()
        return 0

    lax.fori_loop(1, PLANE, send_stat, 0)

    def columns_of(there):
        return w.at[:, pl.ds(pl.multiple_of(there * WIDE, WIDE), WIDE)]

    def index_of(to):
        return to["x"] * NZ + to["z"]

    def send_weight(dx, dz):
        to = device(dx, dz)
        there = index_of(to)

        @pl.when(there < ACTIVE)
        def _():
            columns = columns_of(there)
            if dx == 0 and dz == 0:
                pltpu.make_async_copy(columns, dbuf.at[GRID, me], own_sem.at[0]).start()
            else:
                remote(columns, dbuf.at[GRID, me], send_w.at[0], w_sem.at[me], to).start()

    def along(index):
        return lax.rem(z + index + NZ, NZ)

    def piece(yy, xx, k):
        return abuf.at[lax.rem(yy + NY, NY), lax.rem(xx + NX, NX) * NZ + along(Z_ORDER[k])]

    def pass_on(ref, sem, **to):
        remote(ref, ref, send_piece.at[0], sem, device(**to)).start()

    def up_and_down(ref, n):
        pass_on(ref, yd_sem.at[n], dy=1)
        pass_on(ref, yu_sem.at[n], dy=-1)

    for k in range(NZ):
        ref = piece(y, x, k)
        if k > 0:
            arrived(ref, z_sem.at[k])
        if k == 0 or (k % 2 == 1 and k < 7):
            pass_on(ref, z_sem.at[k + 1 if k == 0 else k + 2], dz=1)
        if k == 0 or (k % 2 == 0 and k < 6):
            pass_on(ref, z_sem.at[k + 2], dz=-1)
        pass_on(ref, xl_sem.at[k], dx=1)
        pass_on(ref, xr_sem.at[k], dx=-1)
        up_and_down(ref, k)
        for item in EARLY[k]:
            send_weight(*item)

    def hear_stat(n, _):
        there = lax.rem(x + n // NZ, NX) * NZ + lax.rem(z + lax.rem(n, NZ), NZ)
        arrived(stat.at[there], stat_sem.at[there])
        return 0

    lax.fori_loop(1, PLANE, hear_stat, 0)
    staty[y] = jnp.sum(stat[...], axis=0)
    for dy in range(1, NY):
        remote(staty.at[y], staty.at[y], send_small.at[1], staty_sem.at[y], device(dy=dy)).start()

    for k in range(NZ):
        left, right = piece(y, x - 1, k), piece(y, x + 1, k)
        arrived(left, xl_sem.at[k])
        if k < 4:
            pass_on(left, x2_sem.at[k], dx=1)
        up_and_down(left, 8 + 2 * k)
        arrived(right, xr_sem.at[k])
        if k >= 4:
            pass_on(right, x2_sem.at[k], dx=-1)
        up_and_down(right, 9 + 2 * k)
        send_weight(2, Z_ORDER[7 - k])
    for k in range(NZ):
        send_weight(3, Z_ORDER[7 - k])
        send_weight(1, Z_ORDER[7 - k])

    for dy in range(1, NY):
        there = lax.rem(y + dy, NY)
        arrived(staty.at[there], staty_sem.at[there])
    channel_mean = staty[...].reshape(PLANE, GROUP) / TOKENS + 1e-06
    own_mean = staty[x, pl.ds(z, 1), :] / TOKENS + 1e-06
    mean_out[...] = own_mean
    log_mean = jnp.log(channel_mean)
    ends[c, 0] = jnp.broadcast_to(jnp.max(log_mean, axis=0, keepdims=True), (8, GROUP))
    ends[c, 1] = jnp.broadcast_to(jnp.min(log_mean, axis=0, keepdims=True), (8, GROUP))
    remote(ends.at[c], ends.at[c], send_small.at[2], ends_sem.at[0], device(dc=1)).start()
    arrived(ends.at[1 - c], ends_sem.at[0])
    top = jnp.max(jnp.maximum(ends[0, 0], ends[1, 0]), axis=(0, 1), keepdims=True)
    bottom = jnp.min(jnp.minimum(ends[0, 1], ends[1, 1]), axis=(0, 1), keepdims=True)
    rows = []
    for k in range(1, GRID):
        ratio = k / GRID
        level = jnp.sqrt(jnp.exp(ratio * top) * jnp.exp(ratio * bottom))
        rows.append(jnp.exp(ratio * log_mean) / level)
    rows.append(jnp.ones((PLANE, GROUP), jnp.float32))
    stacked = jnp.concatenate(rows, axis=0)
    table[...] = stacked.T
    inverse[...] = (1.0 / stacked).T

    def quantize(slot):
        weight = dbuf[GRID, slot].astype(jnp.float32)
        factors = pltpu.roll(table[...], GROUP - slot, 1)
        backs = pltpu.roll(inverse[...], GROUP - slot, 1)
        for k in range(GRID):
            if k == 0:
                scaled = weight
            else:
                at = (k - 1) * PLANE
                scaled = weight * factors[:, at : at + 1]
            step = (jnp.max(jnp.abs(scaled), axis=0, keepdims=True) + 1e-06) * (1.0 / 7.0)
            value = scaled * (1.0 / step)
            whole = jnp.round(value)
            rest = value - whole
            square = rest * rest
            wave = jnp.full_like(square, WAVE[-1])
            for term in WAVE[-2::-1]:
                wave = wave * square + term
            level = whole + rest * square * wave
            result = level * step
            if k > 0:
                result = result * backs[:, at : at + 1]
            dbuf[k, slot] = result.astype(jnp.bfloat16)

    def slot_of(n):
        n = jnp.int32(n)
        order = jnp.where(n < 8, n, jnp.where(n < 24, (n - 8) // 2, n - 24))
        dx = jnp.where(n < 8, 0, jnp.where(n < 24, jnp.where(lax.rem(n, 2) == 0, -1, 1), 2))
        dz = jnp.where(lax.rem(order, 2) == 1, -((order + 1) // 2), order // 2)
        return lax.rem(x + dx + NX, NX) * NZ + lax.rem(z + dz + NZ, NZ)

    def relay(n):
        n = jnp.int32(n)
        slot = slot_of(n)
        below = abuf.at[lax.rem(y + NY - 1, NY), slot]
        above = abuf.at[lax.rem(y + 1, NY), slot]
        arrived(below, yd_sem.at[n])

        @pl.when(lax.rem(n, 2) == 0)
        def _():
            pass_on(below, y2_sem.at[n], dy=1)

        arrived(above, yu_sem.at[n])

        @pl.when(lax.rem(n, 2) == 1)
        def _():
            pass_on(above, y2_sem.at[n], dy=-1)

    def take(i):
        i = jnp.int32(i)
        group, order = i // NZ, NZ - 1 - lax.rem(i, NZ)
        dx = jnp.where(group < 2, jnp.where(group == 0, X_ORDER[0], X_ORDER[1]), jnp.where(group == 2, X_ORDER[2], X_ORDER[3]))
        dz = jnp.where(lax.rem(order, 2) == 1, -((order + 1) // 2), order // 2)
        slot = lax.rem(x - dx + NX, NX) * NZ + lax.rem(z - dz + NZ, NZ)

        @pl.when(active)
        def _():
            @pl.when(slot == me)
            def _():
                pltpu.make_async_copy(dbuf.at[GRID, slot], dbuf.at[GRID, slot], own_sem.at[0]).wait()

            @pl.when(slot != me)
            def _():
                arrived(dbuf.at[GRID, slot], w_sem.at[slot])

            quantize(slot)

    def last(n, _):
        arrived(abuf.at[lax.rem(y + 2, NY), slot_of(n)], y2_sem.at[n])
        return 0

    def multiply(block, k):
        lhs = abuf[block].reshape(TOKENS, HALF)
        rhs = dbuf[k, pl.ds(block * SUB, SUB)].reshape(HALF, WIDE)
        return jnp.dot(lhs, rhs, preferred_element_type=jnp.float32)

    final = lax.rem(y + 2, NY)

    def near(group):
        block = lax.rem(x - X_ORDER[group] + NX, NX)

        @pl.when(jnp.logical_and(active, block != final))
        def _():
            def more(k, _):
                acc[k] += multiply(block, k)
                return 0

            lax.fori_loop(0, GRID + 1, more, 0)

    for k in range(NZ):
        far = piece(y, x + 2, k)
        arrived(far, x2_sem.at[k])
        up_and_down(far, 24 + k)
        relay(2 * k)
        relay(2 * k + 1)
        take(k)

    def both(i, _):
        relay(2 * i)
        relay(2 * i + 1)
        take(i)
        return 0

    def rest(i, _):
        take(i)
        return 0

    lax.fori_loop(NZ, 2 * NZ, both, 0)
    near(0)
    near(1)
    lax.fori_loop(2 * NZ, 3 * NZ, rest, 0)
    near(2)
    lax.fori_loop(3 * NZ, 4 * NZ, rest, 0)
    near(3)
    lax.fori_loop(0, PLANE, last, 0)

    @pl.when(active)
    def _():
        acc[GRID] += multiply(final, GRID)

        def finish(k, _):
            residue = acc[k] + multiply(final, k) - acc[GRID]
            part[k, 0] = residue[:, :GROUP]
            part[k, 1] = residue[:, GROUP:]
            remote(part.at[k, 1 - c], other.at[k], send_part.at[0], part_sem.at[k], device(dc=1)).start()
            return 0

        lax.fori_loop(0, GRID, finish, 0)
        sums = []
        for k in range(GRID):
            arrived(other.at[k], part_sem.at[k])
            residue = part[k, c] + other[k]
            sums.append(jnp.sum(residue * residue, axis=0, keepdims=True))
        mine[...] = jnp.concatenate(sums + [jnp.zeros((GRID, GROUP), jnp.float32)], axis=0)

    @pl.when(jnp.logical_not(active))
    def _():
        mine[...] = jnp.zeros((8, GROUP), jnp.float32)

    tile = 2 * me + c
    owner = (tile // 7) * 8 + lax.rem(tile, 7)

    def send_tile(to_index, slot):
        to = {"x": to_index // (NZ * NC), "z": lax.rem(to_index // NC, NZ), "c": lax.rem(to_index, NC), "y": y}
        same = to_index == tile

        @pl.when(jnp.logical_not(same))
        def _():
            remote(mine, tiles.at[slot], send_small.at[3], tile_sem.at[slot], to).start()

        @pl.when(same)
        def _():
            tiles[slot] = mine[...]

    @pl.when(active)
    def _():
        send_tile(owner, 1)
        send_tile(owner + 1, 0)

    finals[me] = mine[...]

    def send_final(n, _):
        remote(finals.at[me], finals.at[me], send_small.at[4], fin_sem.at[me], device(n // NZ, lax.rem(n, NZ))).start()
        return 0

    lax.fori_loop(1, PLANE, send_final, 0)

    place = lax.rem(tile, 8)
    before = (tile // 8) * 7 + place - 1
    after = before + 1

    @pl.when(jnp.logical_and(place > 0, before != tile))
    def _():
        arrived(tiles.at[0], tile_sem.at[0])

    @pl.when(place == 0)
    def _():
        tiles[0] = jnp.zeros((8, GROUP), jnp.float32)

    @pl.when(jnp.logical_and(place < 7, after != tile))
    def _():
        arrived(tiles.at[1], tile_sem.at[1])

    @pl.when(place == 7)
    def _():
        tiles[1] = jnp.zeros((8, GROUP), jnp.float32)

    shift = 16 * place
    lane = lax.broadcasted_iota(jnp.int32, (8, GROUP), 1)
    joined = jnp.where(lane < shift, pltpu.roll(tiles[0], shift, 1), pltpu.roll(tiles[1], shift, 1))
    cols_out[...] = joined / TOKENS

    def hear_final(n, _):
        there = lax.rem(x + n // NZ, NX) * NZ + lax.rem(z + lax.rem(n, NZ), NZ)
        arrived(finals.at[there], fin_sem.at[there])
        return 0

    lax.fori_loop(1, PLANE, hear_final, 0)
    place_yc = 2 * y + c
    finaly[place_yc] = jnp.sum(finals[...], axis=0)
    for n in range(1, NY * NC):
        to = device(dy=n // NC, dc=n % NC)
        remote(finaly.at[place_yc], finaly.at[place_yc], send_small.at[4], finy_sem.at[place_yc], to).start()
    for n in range(1, NY * NC):
        there = 2 * lax.rem(y + n // NC, NY) + lax.rem(c + n % NC, NC)
        arrived(finaly.at[there], finy_sem.at[there])
    total = jnp.sum(jnp.sum(finaly[...], axis=0), axis=1, keepdims=True)
    errors_out[...] = jnp.broadcast_to(total / (TOKENS * F), (8, GROUP))

    for j in range(SUB):
        arrived(swap.at[j], send_small.at[0])

    def left_stat(n, _):
        arrived(stat.at[0], send_small.at[1])
        return 0

    lax.fori_loop(0, PLANE - 1 + NY - 1, left_stat, 0)
    arrived(ends.at[0], send_small.at[2])

    @pl.when(active)
    def _():
        @pl.when(owner != tile)
        def _():
            arrived(mine, send_small.at[3])

        @pl.when(owner + 1 != tile)
        def _():
            arrived(mine, send_small.at[3])

        for k in range(GRID):
            arrived(other.at[0], send_part.at[0])

    def left_final(n, _):
        arrived(finals.at[0], send_small.at[4])
        return 0

    lax.fori_loop(0, PLANE - 1 + NY * NC - 1, left_final, 0)

    def left_piece(n, _):
        arrived(abuf.at[0, 0], send_piece.at[0])
        return 0

    lax.fori_loop(0, NZ - 1 + 2 * NZ + NZ + 2 * PLANE + PLANE, left_piece, 0)

    def left_weight(n, _):
        arrived(dbuf.at[GRID, 0], send_w.at[0])
        return 0

    lax.fori_loop(0, jnp.where(active, ACTIVE - 1, ACTIVE), left_weight, 0)


def on_device(activations, weight):
    vmem = pl.BlockSpec(memory_space=pltpu.VMEM)
    dma = pltpu.SemaphoreType.DMA
    f32, bf16 = jnp.float32, jnp.bfloat16
    own_mean, cols, errors = pl.pallas_call(
        kernel,
        out_shape=(
            jax.ShapeDtypeStruct((1, GROUP), f32),
            jax.ShapeDtypeStruct((8, GROUP), f32),
            jax.ShapeDtypeStruct((8, GROUP), f32),
        ),
        in_specs=[vmem, pl.BlockSpec(memory_space=pl.ANY)],
        out_specs=(vmem, vmem, vmem),
        scratch_shapes=[
            pltpu.VMEM((SUB, ROWS // 2, GROUP), bf16),
            pltpu.VMEM((NY, PLANE, ROWS, HALF), bf16),
            pltpu.VMEM((GRID + 1, PLANE, GROUP, WIDE), bf16),
            pltpu.VMEM((GRID + 1, TOKENS, WIDE), f32),
            pltpu.VMEM((GRID, NC, TOKENS, GROUP), f32),
            pltpu.VMEM((GRID, TOKENS, GROUP), f32),
            pltpu.VMEM((PLANE, 8, GROUP), f32),
            pltpu.VMEM((NY, 8, GROUP), f32),
            pltpu.VMEM((NC, 2, 8, GROUP), f32),
            pltpu.VMEM((GROUP, GROUP), f32),
            pltpu.VMEM((GROUP, GROUP), f32),
            pltpu.VMEM((2, 8, GROUP), f32),
            pltpu.VMEM((8, GROUP), f32),
            pltpu.VMEM((PLANE, 8, GROUP), f32),
            pltpu.VMEM((NY * NC, 8, GROUP), f32),
            dma((5,)),
            dma((1,)),
            dma((1,)),
            dma((1,)),
            dma((SUB,)),
            dma((NZ,)),
            dma((NZ,)),
            dma((NZ,)),
            dma((NZ,)),
            dma((PLANE,)),
            dma((PLANE,)),
            dma((PLANE,)),
            dma((PLANE,)),
            dma((PLANE,)),
            dma((NY,)),
            dma((1,)),
            dma((GRID,)),
            dma((2,)),
            dma((PLANE,)),
            dma((NY * NC,)),
            dma((1,)),
        ],
        compiler_params=pltpu.CompilerParams(
            collective_id=0, has_side_effects=True, vmem_limit_bytes=60 * 1024 * 1024
        ),
    )(activations, weight)
    return own_mean[0], cols[:GRID, :112], errors[:GRID, 0]


def solution(mesh):
    torus = Mesh(mesh.devices.reshape(NX, NZ, NC, NY), ("x", "z", "c", "y"))
    placed = (P(DP, "y"), P(DP, "y"))
    return jax.shard_map(
        on_device,
        mesh=torus,
        in_specs=placed,
        out_specs=(P(DP), P(None, ("y", "x", "z", "c")), P()),
        check_vma=False,
    )
```

```python
import functools

import jax
import jax.numpy as jnp
from jax import lax
from jax.experimental import pallas as pl
from jax.experimental.pallas import tpu as pltpu
from jax.sharding import Mesh
from jax.sharding import PartitionSpec as P

D = 8192
F = 28672
GROUP = 128
GRID = 4
TOKENS = 768
NX, NZ, NC, NY = 4, 8, 2, 4
PLANE = NX * NZ
ACTIVE = 28
ROWS = 24
HALF = 1024
WIDE = 256
SUB = HALF // GROUP
DP = ("x", "z", "c")
Z_ORDER = (0, -1, 1, -2, 2, -3, 3, -4)
X_ORDER = ((2, 0), (3, 1))
WAVE = (6.579736255173805, -12.987875283620534, 12.207951996649596, -6.691021837978725, 2.380346767313312, -0.5278301996489366)
FIRST = 6
REST = NZ - FIRST
MESH_ID = pl.DeviceIdType.MESH


def kernel(
    act, w, out,
    swap, abuf, dbuf, acc, part, other, stat, staty, ends, table, inverse, tiles, mine, finals, finaly,
    send_small, send_piece, send_w, send_part,
    swap_sem, z_sem, xl_sem, xr_sem, x2_sem, yd_sem, yu_sem, y2_sem, qd_sem, qu_sem, q2_sem, ql_sem, qr_sem, qf_sem, w_sem, stat_sem, staty_sem, ends_sem,
    part_sem, tile_sem, fin_sem, finy_sem, own_sem,
):
    x, z, c, y = (lax.axis_index(name) for name in ("x", "z", "c", "y"))
    me = x * NZ + z
    def works(chip):
        return lax.rem(chip, 10) != 1

    def pair_of(chip):
        return chip - (chip + 8) // 10

    active = works(me)

    def device(dx=0, dz=0, dc=0, dy=0):
        return {
            "x": lax.rem(x + dx + NX, NX),
            "z": lax.rem(z + dz + NZ, NZ),
            "c": lax.rem(c + dc, NC),
            "y": lax.rem(y + dy + NY, NY),
        }

    def remote(src, dst, send, recv, to):
        return pltpu.make_async_remote_copy(
            src_ref=src, dst_ref=dst, send_sem=send, recv_sem=recv, device_id=to, device_id_type=MESH_ID
        )

    def arrived(ref, sem):
        pltpu.make_async_copy(ref, ref, sem).wait()

    barrier = pltpu.get_barrier_semaphore()

    def greet(n, _):
        to = device(n // (NZ * NC), lax.rem(n // NC, NZ), lax.rem(n, NC))
        pl.semaphore_signal(barrier, inc=1, device_id=to, device_id_type=MESH_ID)
        return 0

    lax.fori_loop(1, PLANE * NC, greet, 0)
    for dy in range(1, NY):
        for dc in range(NC):
            pl.semaphore_signal(barrier, inc=1, device_id=device(dy=dy, dc=dc), device_id_type=MESH_ID)
    for k in range(GRID + 1):
        acc[k] = jnp.zeros((TOKENS, WIDE), jnp.float32)
    pl.semaphore_wait(barrier, PLANE * NC - 1 + (NY - 1) * NC)

    def lanes(group):
        return pl.ds(pl.multiple_of(group * GROUP, GROUP), GROUP)

    for j in range(SUB):
        remote(
            act.at[:, lanes(2 * j + 1 - c)], swap.at[j], send_small.at[0], swap_sem.at[j], device(dc=1)
        ).start()
    here = c == 0
    out[...] = jnp.zeros((16, GROUP), jnp.float32)
    for j in range(SUB):
        arrived(swap.at[j], swap_sem.at[j])
        own = act[:, lanes(2 * j + c)].astype(jnp.float32)
        peer = swap[j].astype(jnp.float32)
        block = jnp.concatenate([jnp.where(here, own, peer), jnp.where(here, peer, own)], axis=0)
        stat[me, j : j + 1, :] = jnp.sum(jnp.abs(block), axis=0, keepdims=True)
        abuf[y, me, :, j * GROUP : (j + 1) * GROUP] = block.astype(jnp.bfloat16)

    def send_stat(n, _):
        to = device(n // NZ, lax.rem(n, NZ))
        remote(stat.at[me], stat.at[me], send_small.at[1], stat_sem.at[me], to).start()
        return 0

    lax.fori_loop(1, PLANE, send_stat, 0)

    def columns_of(pair):
        return w.at[:, pl.ds(pl.multiple_of(pair * WIDE, WIDE), WIDE)]

    def index_of(to):
        return to["x"] * NZ + to["z"]

    def send_weight(dx, dz):
        to = device(dx, dz)
        there = index_of(to)

        @pl.when(works(there))
        def _():
            columns = columns_of(pair_of(there))
            if dx == 0 and dz == 0:
                pltpu.make_async_copy(columns, dbuf.at[GRID, me], own_sem.at[0]).start()
            else:
                remote(columns, dbuf.at[GRID, me], send_w.at[0], w_sem.at[me], to).start()

    def along(index):
        return lax.rem(z + index + NZ, NZ)

    def piece(yy, xx, k):
        return abuf.at[lax.rem(yy + NY, NY), lax.rem(xx + NX, NX) * NZ + along(Z_ORDER[k])]

    def pass_on(ref, sem, **to):
        remote(ref, ref, send_piece.at[0], sem, device(**to)).start()

    def up_and_down(ref, n):
        pass_on(ref, yd_sem.at[n], dy=1)
        pass_on(ref, yu_sem.at[n], dy=-1)

    def hear_stat(n, _):
        there = lax.rem(x + n // NZ, NX) * NZ + lax.rem(z + lax.rem(n, NZ), NZ)
        arrived(stat.at[there], stat_sem.at[there])
        return 0

    def left_and_right(ref, m):
        pass_on(ref, ql_sem.at[m], dx=1)
        pass_on(ref, qr_sem.at[m], dx=-1)

    for k in range(NZ):
        ref = piece(y, x, k)
        if k == 0:
            for n in range(1, NZ):
                pass_on(ref, z_sem.at[n], dz=-Z_ORDER[n])
        else:
            arrived(ref, z_sem.at[k])
        if k < FIRST:
            pass_on(ref, xl_sem.at[k], dx=1)
            pass_on(ref, xr_sem.at[k], dx=-1)
            up_and_down(ref, k)
        else:
            pass_on(ref, qd_sem.at[k - FIRST], dy=1)
            pass_on(ref, qu_sem.at[k - FIRST], dy=-1)
            left_and_right(ref, k - FIRST)
        for dx in X_ORDER[0]:
            send_weight(dx, Z_ORDER[7 - k])
        if k == 2:
            lax.fori_loop(1, PLANE, hear_stat, 0)
            staty[y] = jnp.sum(stat[...], axis=0)
            for dy in range(1, NY):
                remote(staty.at[y], staty.at[y], send_small.at[1], staty_sem.at[y], device(dy=dy)).start()

    for k in range(FIRST):
        left, right = piece(y, x - 1, k), piece(y, x + 1, k)
        arrived(left, xl_sem.at[k])
        if k < FIRST // 2:
            pass_on(left, x2_sem.at[k], dx=1)
        up_and_down(left, FIRST + 2 * k)
        arrived(right, xr_sem.at[k])
        if k >= FIRST // 2:
            pass_on(right, x2_sem.at[k], dx=-1)
        up_and_down(right, FIRST + 1 + 2 * k)
    for q in range(REST):
        below, above = piece(y - 1, x, FIRST + q), piece(y + 1, x, FIRST + q)
        arrived(below, qd_sem.at[q])
        if q < REST // 2:
            pass_on(below, q2_sem.at[q], dy=1)
        left_and_right(below, REST + 2 * q)
        arrived(above, qu_sem.at[q])
        if q >= REST // 2:
            pass_on(above, q2_sem.at[q], dy=-1)
        left_and_right(above, REST + 1 + 2 * q)

    for dy in range(1, NY):
        there = lax.rem(y + dy, NY)
        arrived(staty.at[there], staty_sem.at[there])
    channel_mean = staty[...].reshape(PLANE, GROUP) / TOKENS + 1e-06
    own_mean = staty[x, pl.ds(z, 1), :] / TOKENS + 1e-06
    out[8:9, :] = own_mean
    log_mean = jnp.log(channel_mean)
    ends[c, 0] = jnp.broadcast_to(jnp.max(log_mean, axis=0, keepdims=True), (8, GROUP))
    ends[c, 1] = jnp.broadcast_to(jnp.min(log_mean, axis=0, keepdims=True), (8, GROUP))
    remote(ends.at[c], ends.at[c], send_small.at[2], ends_sem.at[0], device(dc=1)).start()
    arrived(ends.at[1 - c], ends_sem.at[0])
    top = jnp.max(jnp.maximum(ends[0, 0], ends[1, 0]), axis=(0, 1), keepdims=True)
    bottom = jnp.min(jnp.minimum(ends[0, 1], ends[1, 1]), axis=(0, 1), keepdims=True)
    rows = []
    for k in range(1, GRID):
        ratio = k / GRID
        level = jnp.sqrt(jnp.exp(ratio * top) * jnp.exp(ratio * bottom))
        rows.append(jnp.exp(ratio * log_mean) / level)
    rows.append(jnp.ones((PLANE, GROUP), jnp.float32))
    stacked = jnp.concatenate(rows, axis=0)
    table[...] = stacked.T
    inverse[...] = (1.0 / stacked).T

    def quantize(slot):
        weight = dbuf[GRID, slot].astype(jnp.float32)
        factors = pltpu.roll(table[...], GROUP - slot, 1)
        backs = pltpu.roll(inverse[...], GROUP - slot, 1)
        for k in range(GRID):
            if k == 0:
                scaled = weight
            else:
                at = (k - 1) * PLANE
                scaled = weight * factors[:, at : at + 1]
            step = (jnp.max(jnp.abs(scaled), axis=0, keepdims=True) + 1e-06) * (1.0 / 7.0)
            value = scaled * (1.0 / step)
            whole = jnp.round(value)
            rest = value - whole
            square = rest * rest
            wave = jnp.full_like(square, WAVE[-1])
            for term in WAVE[-2::-1]:
                wave = wave * square + term
            level = whole + rest * square * wave
            result = level * step
            if k > 0:
                result = result * backs[:, at : at + 1]
            dbuf[k, slot] = result.astype(jnp.bfloat16)

    def slot_of(n):
        n = jnp.int32(n)
        order = jnp.where(n < FIRST, n, jnp.where(n < 3 * FIRST, (n - FIRST) // 2, n - 3 * FIRST))
        beside = jnp.where(lax.rem(n - FIRST + NX * NZ, 2) == 0, -1, 1)
        dx = jnp.where(n < FIRST, 0, jnp.where(n < 3 * FIRST, beside, 2))
        dz = jnp.where(lax.rem(order, 2) == 1, -((order + 1) // 2), order // 2)
        return lax.rem(x + dx + NX, NX) * NZ + lax.rem(z + dz + NZ, NZ)

    def relay(n):
        n = jnp.int32(n)
        slot = slot_of(n)
        below = abuf.at[lax.rem(y + NY - 1, NY), slot]
        above = abuf.at[lax.rem(y + 1, NY), slot]
        arrived(below, yd_sem.at[n])

        @pl.when(lax.rem(n, 2) == 0)
        def _():
            pass_on(below, y2_sem.at[n], dy=1)

        arrived(above, yu_sem.at[n])

        @pl.when(lax.rem(n, 2) == 1)
        def _():
            pass_on(above, y2_sem.at[n], dy=-1)

    def take(i):
        i = jnp.int32(i)
        first, even = i < 2 * NZ, lax.rem(i, 2) == 0
        order = NZ - 1 - lax.rem(i // 2, NZ)
        dx = jnp.where(first, jnp.where(even, X_ORDER[0][0], X_ORDER[0][1]), jnp.where(even, X_ORDER[1][0], X_ORDER[1][1]))
        dz = jnp.where(lax.rem(order, 2) == 1, -((order + 1) // 2), order // 2)
        slot = lax.rem(x - dx + NX, NX) * NZ + lax.rem(z - dz + NZ, NZ)

        @pl.when(active)
        def _():
            @pl.when(slot == me)
            def _():
                pltpu.make_async_copy(dbuf.at[GRID, slot], dbuf.at[GRID, slot], own_sem.at[0]).wait()

            @pl.when(slot != me)
            def _():
                arrived(dbuf.at[GRID, slot], w_sem.at[slot])

            quantize(slot)

    def last(n, _):
        arrived(abuf.at[lax.rem(y + 2, NY), slot_of(n)], y2_sem.at[n])
        return 0

    def multiply(block, k):
        lhs = abuf[block].reshape(TOKENS, HALF)
        rhs = dbuf[k, pl.ds(block * SUB, SUB)].reshape(HALF, WIDE)
        return jnp.dot(lhs, rhs, preferred_element_type=jnp.float32)

    def accumulate(block):
        for k in range(GRID + 1):
            acc[k] += multiply(block, k)

    later = [(dx, Z_ORDER[7 - k]) for k in range(NZ) for dx in X_ORDER[1]]
    for k in range(FIRST):
        far = piece(y, x + 2, k)
        arrived(far, x2_sem.at[k])
        up_and_down(far, 3 * FIRST + k)
        for n in range(3 * k, 3 * k + 3):
            relay(n)
        for item in later[3 * k : 3 * k + 3]:
            send_weight(*item)
        take(k)
    for q in range(REST):
        across = piece(y + 2, x, FIRST + q)
        arrived(across, q2_sem.at[q])
        left_and_right(across, 3 * REST + q)
        take(FIRST + q)

    def side(m, dx):
        q = m if m < REST else (m - REST) // 2 if m < 3 * REST else m - 3 * REST
        dy = 0 if m < REST else (1 if (m - REST) % 2 else -1) if m < 3 * REST else 2
        return piece(y + dy, x + dx, FIRST + q)

    def beside(m):
        arrived(side(m, -1), ql_sem.at[m])
        if m % 2 == 0:
            pass_on(side(m, -1), qf_sem.at[m], dx=1)
        arrived(side(m, 1), qr_sem.at[m])
        if m % 2 == 1:
            pass_on(side(m, 1), qf_sem.at[m], dx=-1)

    for m in range(2 * REST):
        beside(m)

    def two(j, _):
        relay(3 * FIRST + j)
        take(NZ + j)
        return 0

    def one(i, _):
        take(i)
        return 0

    lax.fori_loop(0, FIRST, two, 0)
    for m in range(2 * REST, 3 * REST):
        beside(m)
    lax.fori_loop(NZ + FIRST, 2 * NZ, one, 0)
    for m in range(3 * REST, 4 * REST):
        beside(m)
    for m in range(3 * REST):
        arrived(side(m, 2), qf_sem.at[m])
    opposite = lax.rem(x - y + NX, NX) == 2
    sooner = lax.rem(jnp.where(opposite, x + 2, x), NX)
    later_one = lax.rem(jnp.where(opposite, x, x + 2), NX)

    @pl.when(active)
    def _():
        accumulate(sooner)

    lax.fori_loop(2 * NZ, 3 * NZ + 4, one, 0)
    lax.fori_loop(0, NX * FIRST, last, 0)
    for m in range(3 * REST, 4 * REST):
        arrived(side(m, 2), qf_sem.at[m])

    @pl.when(active)
    def _():
        accumulate(later_one)

    lax.fori_loop(3 * NZ + 4, 4 * NZ, one, 0)
    final = lax.rem(x + NX - 1, NX)

    @pl.when(active)
    def _():
        accumulate(lax.rem(x + 1, NX))
        acc[GRID] += multiply(final, GRID)
        for k in range(GRID):
            residue = acc[k] + multiply(final, k) - acc[GRID]
            part[k, 0] = residue[:, :GROUP]
            part[k, 1] = residue[:, GROUP:]
            remote(part.at[k, 1 - c], other.at[k], send_part.at[0], part_sem.at[k], device(dc=1)).start()
        sums = []
        for k in range(GRID):
            arrived(other.at[k], part_sem.at[k])
            residue = part[k, c] + other[k]
            sums.append(jnp.sum(residue * residue, axis=0, keepdims=True))
        mine[...] = jnp.concatenate(sums + [jnp.zeros((GRID, GROUP), jnp.float32)], axis=0)

    @pl.when(jnp.logical_not(active))
    def _():
        mine[...] = jnp.zeros((8, GROUP), jnp.float32)

    seat = 2 * me + c
    tile = 2 * pair_of(me) + c
    owner = (tile // 7) * 8 + lax.rem(tile, 7)

    def send_tile(to_index, slot):
        to = {"x": to_index // (NZ * NC), "z": lax.rem(to_index // NC, NZ), "c": lax.rem(to_index, NC), "y": y}
        same = to_index == seat

        @pl.when(jnp.logical_not(same))
        def _():
            remote(mine, tiles.at[slot], send_small.at[3], tile_sem.at[slot], to).start()

        @pl.when(same)
        def _():
            tiles[slot] = mine[...]

    @pl.when(active)
    def _():
        send_tile(owner, 1)
        send_tile(owner + 1, 0)

    finals[me] = mine[...]

    def send_final(n, _):
        remote(finals.at[me], finals.at[me], send_small.at[4], fin_sem.at[me], device(n // NZ, lax.rem(n, NZ))).start()
        return 0

    lax.fori_loop(1, PLANE, send_final, 0)

    place = lax.rem(seat, 8)
    before = (seat // 8) * 7 + place - 1
    after = before + 1

    def from_other(source):
        return jnp.logical_not(jnp.logical_and(active, source == tile))

    @pl.when(jnp.logical_and(place > 0, from_other(before)))
    def _():
        arrived(tiles.at[0], tile_sem.at[0])

    @pl.when(place == 0)
    def _():
        tiles[0] = jnp.zeros((8, GROUP), jnp.float32)

    @pl.when(jnp.logical_and(place < 7, from_other(after)))
    def _():
        arrived(tiles.at[1], tile_sem.at[1])

    @pl.when(place == 7)
    def _():
        tiles[1] = jnp.zeros((8, GROUP), jnp.float32)

    shift = 16 * place
    lane = lax.broadcasted_iota(jnp.int32, (8, GROUP), 1)
    joined = jnp.where(lane < shift, pltpu.roll(tiles[0], shift, 1), pltpu.roll(tiles[1], shift, 1))
    out[0:8, :] = joined / TOKENS

    def hear_final(n, _):
        there = lax.rem(x + n // NZ, NX) * NZ + lax.rem(z + lax.rem(n, NZ), NZ)
        arrived(finals.at[there], fin_sem.at[there])
        return 0

    lax.fori_loop(1, PLANE, hear_final, 0)
    place_yc = 2 * y + c
    finaly[place_yc] = jnp.sum(finals[...], axis=0)
    for n in range(1, NY * NC):
        to = device(dy=n // NC, dc=n % NC)
        remote(finaly.at[place_yc], finaly.at[place_yc], send_small.at[4], finy_sem.at[place_yc], to).start()
    for n in range(1, NY * NC):
        there = 2 * lax.rem(y + n // NC, NY) + lax.rem(c + n % NC, NC)
        arrived(finaly.at[there], finy_sem.at[there])
    total = jnp.sum(jnp.sum(finaly[...], axis=0), axis=1, keepdims=True)
    row = lax.broadcasted_iota(jnp.int32, (8, GROUP), 0)
    spread = jnp.where(row == lane, jnp.broadcast_to(total / (TOKENS * F), (8, GROUP)), 0.0)
    out[9:10, :] = jnp.sum(spread, axis=0, keepdims=True)

    for j in range(SUB):
        arrived(swap.at[j], send_small.at[0])

    def left_stat(n, _):
        arrived(stat.at[0], send_small.at[1])
        return 0

    lax.fori_loop(0, PLANE - 1 + NY - 1, left_stat, 0)
    arrived(ends.at[0], send_small.at[2])

    @pl.when(active)
    def _():
        @pl.when(owner != seat)
        def _():
            arrived(mine, send_small.at[3])

        @pl.when(owner + 1 != seat)
        def _():
            arrived(mine, send_small.at[3])

        for k in range(GRID):
            arrived(other.at[0], send_part.at[0])

    def left_final(n, _):
        arrived(finals.at[0], send_small.at[4])
        return 0

    lax.fori_loop(0, PLANE - 1 + NY * NC - 1, left_final, 0)

    def left_piece(n, _):
        arrived(abuf.at[0, 0], send_piece.at[0])
        return 0

    lax.fori_loop(0, NZ - 1 + 2 * NZ + NZ + 2 * PLANE + PLANE, left_piece, 0)

    def left_weight(n, _):
        arrived(dbuf.at[GRID, 0], send_w.at[0])
        return 0

    lax.fori_loop(0, jnp.where(active, ACTIVE - 1, ACTIVE), left_weight, 0)


def unpack(packed, mean_out, cols_out, errors_out):
    mean_out[...] = packed[8, :]
    cols_out[...] = packed[:GRID, : cols_out.shape[1]]
    errors_out[...] = packed[9, :GRID]


def on_device(activations, weight):
    vmem = pl.BlockSpec(memory_space=pltpu.VMEM)
    dma = pltpu.SemaphoreType.DMA
    f32, bf16 = jnp.float32, jnp.bfloat16
    packed = pl.pallas_call(
        kernel,
        out_shape=jax.ShapeDtypeStruct((16, GROUP), f32),
        in_specs=[vmem, pl.BlockSpec(memory_space=pl.ANY)],
        out_specs=vmem,
        scratch_shapes=[
            pltpu.VMEM((SUB, ROWS // 2, GROUP), bf16),
            pltpu.VMEM((NY, PLANE, ROWS, HALF), bf16),
            pltpu.VMEM((GRID + 1, PLANE, GROUP, WIDE), bf16),
            pltpu.VMEM((GRID + 1, TOKENS, WIDE), f32),
            pltpu.VMEM((GRID, NC, TOKENS, GROUP), f32),
            pltpu.VMEM((GRID, TOKENS, GROUP), f32),
            pltpu.VMEM((PLANE, 8, GROUP), f32),
            pltpu.VMEM((NY, 8, GROUP), f32),
            pltpu.VMEM((NC, 2, 8, GROUP), f32),
            pltpu.VMEM((GROUP, GROUP), f32),
            pltpu.VMEM((GROUP, GROUP), f32),
            pltpu.VMEM((2, 8, GROUP), f32),
            pltpu.VMEM((8, GROUP), f32),
            pltpu.VMEM((PLANE, 8, GROUP), f32),
            pltpu.VMEM((NY * NC, 8, GROUP), f32),
            dma((5,)),
            dma((1,)),
            dma((1,)),
            dma((1,)),
            dma((SUB,)),
            dma((NZ,)),
            dma((NZ,)),
            dma((NZ,)),
            dma((NZ,)),
            dma((NX * FIRST,)),
            dma((NX * FIRST,)),
            dma((NX * FIRST,)),
            dma((REST,)),
            dma((REST,)),
            dma((REST,)),
            dma((NY * REST,)),
            dma((NY * REST,)),
            dma((NY * REST,)),
            dma((PLANE,)),
            dma((PLANE,)),
            dma((NY,)),
            dma((1,)),
            dma((GRID,)),
            dma((2,)),
            dma((PLANE,)),
            dma((NY * NC,)),
            dma((1,)),
        ],
        compiler_params=pltpu.CompilerParams(
            collective_id=0, has_side_effects=True, vmem_limit_bytes=60 * 1024 * 1024
        ),
    )(activations, weight)
    return pl.pallas_call(
        unpack,
        out_shape=(
            jax.ShapeDtypeStruct((GROUP,), f32),
            jax.ShapeDtypeStruct((GRID, F // (PLANE * NC * NY)), f32),
            jax.ShapeDtypeStruct((GRID,), f32),
        ),
        in_specs=[vmem],
        out_specs=(vmem, vmem, vmem),
    )(packed)


def solution(mesh):
    torus = Mesh(mesh.devices.reshape(NX, NZ, NC, NY), ("x", "z", "c", "y"))
    placed = (P(DP, "y"), P(DP, "y"))
    return jax.shard_map(
        on_device,
        mesh=torus,
        in_specs=placed,
        out_specs=(P(DP), P(None, ("y", "x", "z", "c")), P()),
        check_vma=False,
    )
```

```python
import functools

import jax
import jax.numpy as jnp
from jax import lax
from jax.experimental import pallas as pl
from jax.experimental.pallas import tpu as pltpu
from jax.sharding import Mesh
from jax.sharding import PartitionSpec as P

D = 8192
F = 28672
GROUP = 128
GRID = 4
TOKENS = 768
NX, NZ, NC, NY = 4, 8, 2, 4
PLANE = NX * NZ
ACTIVE = 28
ROWS = 24
HALF = 1024
WIDE = 256
SUB = HALF // GROUP
DP = ("x", "z", "c")
Z_ORDER = (0, -1, 1, -2, 2, -3, 3, -4)
X_ORDER = ((2, 0), (3, 1))
WAVE = (6.579736255173805, -12.987875283620534, 12.207951996649596, -6.691021837978725, 2.380346767313312, -0.5278301996489366)
FIRST = 6
REST = NZ - FIRST
MESH_ID = pl.DeviceIdType.MESH


def kernel(
    act, w, out,
    swap, abuf, dbuf, acc, part, other, stat, staty, ends, table, inverse, spread, tiles, mine, finals, finaly,
    send_small, send_piece, send_w, send_part,
    swap_sem, z_sem, xl_sem, xr_sem, x2_sem, yd_sem, yu_sem, y2_sem, qd_sem, qu_sem, q2_sem, ql_sem, qr_sem, qf_sem, w_sem, stat_sem, staty_sem, ends_sem,
    part_sem, tile_sem, fin_sem, finy_sem, own_sem,
):
    x, z, c, y = (lax.axis_index(name) for name in ("x", "z", "c", "y"))
    me = x * NZ + z
    def works(chip):
        return lax.rem(chip, 10) != 1

    def pair_of(chip):
        return chip - (chip + 8) // 10

    active = works(me)

    def device(dx=0, dz=0, dc=0, dy=0):
        return {
            "x": lax.rem(x + dx + NX, NX),
            "z": lax.rem(z + dz + NZ, NZ),
            "c": lax.rem(c + dc, NC),
            "y": lax.rem(y + dy + NY, NY),
        }

    def remote(src, dst, send, recv, to):
        return pltpu.make_async_remote_copy(
            src_ref=src, dst_ref=dst, send_sem=send, recv_sem=recv, device_id=to, device_id_type=MESH_ID
        )

    def arrived(ref, sem):
        pltpu.make_async_copy(ref, ref, sem).wait()

    barrier = pltpu.get_barrier_semaphore()

    def greet(n, _):
        to = device(n // (NZ * NC), lax.rem(n // NC, NZ), lax.rem(n, NC))
        pl.semaphore_signal(barrier, inc=1, device_id=to, device_id_type=MESH_ID)
        return 0

    lax.fori_loop(1, PLANE * NC, greet, 0)
    for dy in range(1, NY):
        for dc in range(NC):
            pl.semaphore_signal(barrier, inc=1, device_id=device(dy=dy, dc=dc), device_id_type=MESH_ID)
    for k in range(GRID + 1):
        acc[k] = jnp.zeros((TOKENS, WIDE), jnp.float32)
    pl.semaphore_wait(barrier, PLANE * NC - 1 + (NY - 1) * NC)

    def lanes(group):
        return pl.ds(pl.multiple_of(group * GROUP, GROUP), GROUP)

    for j in range(SUB):
        remote(
            act.at[:, lanes(2 * j + 1 - c)], swap.at[j], send_small.at[0], swap_sem.at[j], device(dc=1)
        ).start()
    here = c == 0
    out[...] = jnp.zeros((16, GROUP), jnp.float32)
    for j in range(SUB):
        arrived(swap.at[j], swap_sem.at[j])
        own = act[:, lanes(2 * j + c)].astype(jnp.float32)
        peer = swap[j].astype(jnp.float32)
        block = jnp.concatenate([jnp.where(here, own, peer), jnp.where(here, peer, own)], axis=0)
        stat[me, j : j + 1, :] = jnp.sum(jnp.abs(block), axis=0, keepdims=True)
        abuf[y, me, :, j * GROUP : (j + 1) * GROUP] = block.astype(jnp.bfloat16)

    def send_stat(n, _):
        to = device(n // NZ, lax.rem(n, NZ))
        remote(stat.at[me], stat.at[me], send_small.at[1], stat_sem.at[me], to).start()
        return 0

    lax.fori_loop(1, PLANE, send_stat, 0)

    def columns_of(pair):
        return w.at[:, pl.ds(pl.multiple_of(pair * WIDE, WIDE), WIDE)]

    def index_of(to):
        return to["x"] * NZ + to["z"]

    def send_weight(dx, dz):
        to = device(dx, dz)
        there = index_of(to)

        @pl.when(works(there))
        def _():
            columns = columns_of(pair_of(there))
            if dx == 0 and dz == 0:
                pltpu.make_async_copy(columns, dbuf.at[GRID, me], own_sem.at[0]).start()
            else:
                remote(columns, dbuf.at[GRID, me], send_w.at[0], w_sem.at[me], to).start()

    def along(index):
        return lax.rem(z + index + NZ, NZ)

    def piece(yy, xx, k):
        return abuf.at[lax.rem(yy + NY, NY), lax.rem(xx + NX, NX) * NZ + along(Z_ORDER[k])]

    def pass_on(ref, sem, **to):
        remote(ref, ref, send_piece.at[0], sem, device(**to)).start()

    def up_and_down(ref, n):
        pass_on(ref, yd_sem.at[n], dy=1)
        pass_on(ref, yu_sem.at[n], dy=-1)

    def hear_stat(n, _):
        there = lax.rem(x + n // NZ, NX) * NZ + lax.rem(z + lax.rem(n, NZ), NZ)
        arrived(stat.at[there], stat_sem.at[there])
        return 0

    def left_and_right(ref, m):
        pass_on(ref, ql_sem.at[m], dx=1)
        pass_on(ref, qr_sem.at[m], dx=-1)

    for k in range(NZ):
        ref = piece(y, x, k)
        if k == 0:
            for n in range(1, NZ):
                pass_on(ref, z_sem.at[n], dz=-Z_ORDER[n])
        else:
            arrived(ref, z_sem.at[k])
        if k < FIRST:
            pass_on(ref, xl_sem.at[k], dx=1)
            pass_on(ref, xr_sem.at[k], dx=-1)
            up_and_down(ref, k)
        else:
            pass_on(ref, qd_sem.at[k - FIRST], dy=1)
            pass_on(ref, qu_sem.at[k - FIRST], dy=-1)
            left_and_right(ref, k - FIRST)
        for dx in X_ORDER[0]:
            send_weight(dx, Z_ORDER[7 - k])
        if k == 2:
            lax.fori_loop(1, PLANE, hear_stat, 0)
            staty[y] = jnp.sum(stat[...], axis=0)
            for dy in range(1, NY):
                remote(staty.at[y], staty.at[y], send_small.at[1], staty_sem.at[y], device(dy=dy)).start()

    for k in range(FIRST):
        left, right = piece(y, x - 1, k), piece(y, x + 1, k)
        arrived(left, xl_sem.at[k])
        if k < FIRST // 2:
            pass_on(left, x2_sem.at[k], dx=1)
        up_and_down(left, FIRST + 2 * k)
        arrived(right, xr_sem.at[k])
        if k >= FIRST // 2:
            pass_on(right, x2_sem.at[k], dx=-1)
        up_and_down(right, FIRST + 1 + 2 * k)
    for q in range(REST):
        below, above = piece(y - 1, x, FIRST + q), piece(y + 1, x, FIRST + q)
        arrived(below, qd_sem.at[q])
        if q < REST // 2:
            pass_on(below, q2_sem.at[q], dy=1)
        left_and_right(below, REST + 2 * q)
        arrived(above, qu_sem.at[q])
        if q >= REST // 2:
            pass_on(above, q2_sem.at[q], dy=-1)
        left_and_right(above, REST + 1 + 2 * q)

    for dy in range(1, NY):
        there = lax.rem(y + dy, NY)
        arrived(staty.at[there], staty_sem.at[there])
    channel_mean = staty[...].reshape(PLANE, GROUP) / TOKENS + 1e-06
    own_mean = staty[x, pl.ds(z, 1), :] / TOKENS + 1e-06
    out[8:9, :] = own_mean
    log_mean = jnp.log(channel_mean)
    ends[c, 0] = jnp.broadcast_to(jnp.max(log_mean, axis=0, keepdims=True), (8, GROUP))
    ends[c, 1] = jnp.broadcast_to(jnp.min(log_mean, axis=0, keepdims=True), (8, GROUP))
    remote(ends.at[c], ends.at[c], send_small.at[2], ends_sem.at[0], device(dc=1)).start()
    arrived(ends.at[1 - c], ends_sem.at[0])
    top = jnp.max(jnp.maximum(ends[0, 0], ends[1, 0]), axis=(0, 1), keepdims=True)
    bottom = jnp.min(jnp.minimum(ends[0, 1], ends[1, 1]), axis=(0, 1), keepdims=True)
    rows = []
    for k in range(1, GRID):
        ratio = k / GRID
        level = jnp.sqrt(jnp.exp(ratio * top) * jnp.exp(ratio * bottom))
        rows.append(jnp.exp(ratio * log_mean) / level)
    rows.append(jnp.ones((PLANE, GROUP), jnp.float32))
    stacked = jnp.concatenate(rows, axis=0)
    table[...] = stacked.T
    inverse[...] = (1.0 / stacked).T


    def widen(slot):
        factors = pltpu.roll(table[...], GROUP - slot, 1)
        backs = pltpu.roll(inverse[...], GROUP - slot, 1)
        for k in range(GRID - 1):
            at = k * PLANE
            spread[slot, k, 0] = jnp.broadcast_to(factors[:, at : at + 1], (GROUP, GROUP))
            spread[slot, k, 1] = jnp.broadcast_to(backs[:, at : at + 1], (GROUP, GROUP))

    def quantize(slot):
        for half in range(WIDE // GROUP):
            at = slice(half * GROUP, (half + 1) * GROUP)
            weight = dbuf[GRID, slot, :, at].astype(jnp.float32)
            for k in range(GRID):
                scaled = weight if k == 0 else weight * spread[slot, k - 1, 0]
                step = (jnp.max(jnp.abs(scaled), axis=0, keepdims=True) + 1e-06) * (1.0 / 7.0)
                value = scaled * (1.0 / step)
                whole = jnp.round(value)
                rest = value - whole
                square = rest * rest
                wave = jnp.full_like(square, WAVE[-1])
                for term in WAVE[-2::-1]:
                    wave = wave * square + term
                level = whole + rest * square * wave
                result = level * step
                if k > 0:
                    result = result * spread[slot, k - 1, 1]
                dbuf[k, slot, :, at] = result.astype(jnp.bfloat16)

    def slot_of(n):
        n = jnp.int32(n)
        order = jnp.where(n < FIRST, n, jnp.where(n < 3 * FIRST, (n - FIRST) // 2, n - 3 * FIRST))
        beside = jnp.where(lax.rem(n - FIRST + NX * NZ, 2) == 0, -1, 1)
        dx = jnp.where(n < FIRST, 0, jnp.where(n < 3 * FIRST, beside, 2))
        dz = jnp.where(lax.rem(order, 2) == 1, -((order + 1) // 2), order // 2)
        return lax.rem(x + dx + NX, NX) * NZ + lax.rem(z + dz + NZ, NZ)

    def relay(n):
        n = jnp.int32(n)
        slot = slot_of(n)
        below = abuf.at[lax.rem(y + NY - 1, NY), slot]
        above = abuf.at[lax.rem(y + 1, NY), slot]
        arrived(below, yd_sem.at[n])

        @pl.when(lax.rem(n, 2) == 0)
        def _():
            pass_on(below, y2_sem.at[n], dy=1)

        arrived(above, yu_sem.at[n])

        @pl.when(lax.rem(n, 2) == 1)
        def _():
            pass_on(above, y2_sem.at[n], dy=-1)

    def source(i):
        i = jnp.int32(i)
        first, even = i < 2 * NZ, lax.rem(i, 2) == 0
        order = NZ - 1 - lax.rem(i // 2, NZ)
        dx = jnp.where(first, jnp.where(even, X_ORDER[0][0], X_ORDER[0][1]), jnp.where(even, X_ORDER[1][0], X_ORDER[1][1]))
        dz = jnp.where(lax.rem(order, 2) == 1, -((order + 1) // 2), order // 2)
        return lax.rem(x - dx + NX, NX) * NZ + lax.rem(z - dz + NZ, NZ)

    def take(i, wide=True):
        slot = source(i)

        @pl.when(active)
        def _():
            if wide:
                widen(slot)

            @pl.when(slot == me)
            def _():
                pltpu.make_async_copy(dbuf.at[GRID, slot], dbuf.at[GRID, slot], own_sem.at[0]).wait()

            @pl.when(slot != me)
            def _():
                arrived(dbuf.at[GRID, slot], w_sem.at[slot])

            quantize(slot)

    def last(n, _):
        arrived(abuf.at[lax.rem(y + 2, NY), slot_of(n)], y2_sem.at[n])
        return 0

    def multiply(block, k):
        lhs = abuf[block].reshape(TOKENS, HALF)
        rhs = dbuf[k, pl.ds(block * SUB, SUB)].reshape(HALF, WIDE)
        return jnp.dot(lhs, rhs, preferred_element_type=jnp.float32)

    def accumulate(block):
        for k in range(GRID + 1):
            acc[k] += multiply(block, k)

    later = [(dx, Z_ORDER[7 - k]) for k in range(NZ) for dx in X_ORDER[1]]
    for k in range(FIRST):
        far = piece(y, x + 2, k)
        arrived(far, x2_sem.at[k])
        up_and_down(far, 3 * FIRST + k)
        for n in range(3 * k, 3 * k + 3):
            relay(n)
        for item in later[3 * k : 3 * k + 3]:
            send_weight(*item)
        take(k)
    for q in range(REST):
        across = piece(y + 2, x, FIRST + q)
        arrived(across, q2_sem.at[q])
        left_and_right(across, 3 * REST + q)
        take(FIRST + q)

    def side(m, dx):
        q = m if m < REST else (m - REST) // 2 if m < 3 * REST else m - 3 * REST
        dy = 0 if m < REST else (1 if (m - REST) % 2 else -1) if m < 3 * REST else 2
        return piece(y + dy, x + dx, FIRST + q)

    def beside(m):
        arrived(side(m, -1), ql_sem.at[m])
        if m % 2 == 0:
            pass_on(side(m, -1), qf_sem.at[m], dx=1)
        arrived(side(m, 1), qr_sem.at[m])
        if m % 2 == 1:
            pass_on(side(m, 1), qf_sem.at[m], dx=-1)

    for m in range(2 * REST):
        beside(m)

    def two(j, _):
        relay(3 * FIRST + j)

        @pl.when(active)
        def _():
            def ahead(n, _):
                widen(source(n))
                return 0

            lax.fori_loop(2 * NZ + 3 * j, jnp.minimum(2 * NZ + 3 * j + 3, 4 * NZ), ahead, 0)

        take(NZ + j)
        return 0

    def one(i, _):
        take(i, False)
        return 0

    lax.fori_loop(0, FIRST // 2, two, 0)
    for m in range(2 * REST, 3 * REST):
        beside(m)
    lax.fori_loop(FIRST // 2, FIRST, two, 0)
    for m in range(3 * REST, 4 * REST):
        beside(m)
    for i in range(NZ + FIRST, 2 * NZ):
        take(i)
    for m in range(3 * REST):
        arrived(side(m, 2), qf_sem.at[m])
    opposite = lax.rem(x - y + NX, NX) == 2
    sooner = lax.rem(jnp.where(opposite, x + 2, x), NX)
    later_one = lax.rem(jnp.where(opposite, x, x + 2), NX)

    @pl.when(active)
    def _():
        accumulate(sooner)

    lax.fori_loop(2 * NZ, 3 * NZ + 4, one, 0)
    lax.fori_loop(0, NX * FIRST, last, 0)
    for m in range(3 * REST, 4 * REST):
        arrived(side(m, 2), qf_sem.at[m])

    @pl.when(active)
    def _():
        accumulate(later_one)

    lax.fori_loop(3 * NZ + 4, 4 * NZ, one, 0)
    final = lax.rem(x + NX - 1, NX)

    @pl.when(active)
    def _():
        accumulate(lax.rem(x + 1, NX))
        acc[GRID] += multiply(final, GRID)
        for k in range(GRID):
            residue = acc[k] + multiply(final, k) - acc[GRID]
            part[k, 0] = residue[:, :GROUP]
            part[k, 1] = residue[:, GROUP:]
            remote(part.at[k, 1 - c], other.at[k], send_part.at[0], part_sem.at[k], device(dc=1)).start()
        sums = []
        for k in range(GRID):
            arrived(other.at[k], part_sem.at[k])
            residue = part[k, c] + other[k]
            sums.append(jnp.sum(residue * residue, axis=0, keepdims=True))
        mine[...] = jnp.concatenate(sums + [jnp.zeros((GRID, GROUP), jnp.float32)], axis=0)

    @pl.when(jnp.logical_not(active))
    def _():
        mine[...] = jnp.zeros((8, GROUP), jnp.float32)

    seat = 2 * me + c
    tile = 2 * pair_of(me) + c
    owner = (tile // 7) * 8 + lax.rem(tile, 7)

    def send_tile(to_index, slot):
        to = {"x": to_index // (NZ * NC), "z": lax.rem(to_index // NC, NZ), "c": lax.rem(to_index, NC), "y": y}
        same = to_index == seat

        @pl.when(jnp.logical_not(same))
        def _():
            remote(mine, tiles.at[slot], send_small.at[3], tile_sem.at[slot], to).start()

        @pl.when(same)
        def _():
            tiles[slot] = mine[...]

    @pl.when(active)
    def _():
        send_tile(owner, 1)
        send_tile(owner + 1, 0)

    finals[me] = mine[...]

    def send_final(n, _):
        remote(finals.at[me], finals.at[me], send_small.at[4], fin_sem.at[me], device(n // NZ, lax.rem(n, NZ))).start()
        return 0

    lax.fori_loop(1, PLANE, send_final, 0)

    place = lax.rem(seat, 8)
    before = (seat // 8) * 7 + place - 1
    after = before + 1

    def from_other(source):
        return jnp.logical_not(jnp.logical_and(active, source == tile))

    @pl.when(jnp.logical_and(place > 0, from_other(before)))
    def _():
        arrived(tiles.at[0], tile_sem.at[0])

    @pl.when(place == 0)
    def _():
        tiles[0] = jnp.zeros((8, GROUP), jnp.float32)

    @pl.when(jnp.logical_and(place < 7, from_other(after)))
    def _():
        arrived(tiles.at[1], tile_sem.at[1])

    @pl.when(place == 7)
    def _():
        tiles[1] = jnp.zeros((8, GROUP), jnp.float32)

    shift = 16 * place
    lane = lax.broadcasted_iota(jnp.int32, (8, GROUP), 1)
    joined = jnp.where(lane < shift, pltpu.roll(tiles[0], shift, 1), pltpu.roll(tiles[1], shift, 1))
    out[0:8, :] = joined / TOKENS

    def hear_final(n, _):
        there = lax.rem(x + n // NZ, NX) * NZ + lax.rem(z + lax.rem(n, NZ), NZ)
        arrived(finals.at[there], fin_sem.at[there])
        return 0

    lax.fori_loop(1, PLANE, hear_final, 0)
    place_yc = 2 * y + c
    finaly[place_yc] = jnp.sum(finals[...], axis=0)
    for n in range(1, NY * NC):
        to = device(dy=n // NC, dc=n % NC)
        remote(finaly.at[place_yc], finaly.at[place_yc], send_small.at[4], finy_sem.at[place_yc], to).start()
    for n in range(1, NY * NC):
        there = 2 * lax.rem(y + n // NC, NY) + lax.rem(c + n % NC, NC)
        arrived(finaly.at[there], finy_sem.at[there])
    total = jnp.sum(jnp.sum(finaly[...], axis=0), axis=1, keepdims=True)
    row = lax.broadcasted_iota(jnp.int32, (8, GROUP), 0)
    placed = jnp.where(row == lane, jnp.broadcast_to(total / (TOKENS * F), (8, GROUP)), 0.0)
    out[9:10, :] = jnp.sum(placed, axis=0, keepdims=True)

    for j in range(SUB):
        arrived(swap.at[j], send_small.at[0])

    def left_stat(n, _):
        arrived(stat.at[0], send_small.at[1])
        return 0

    lax.fori_loop(0, PLANE - 1 + NY - 1, left_stat, 0)
    arrived(ends.at[0], send_small.at[2])

    @pl.when(active)
    def _():
        @pl.when(owner != seat)
        def _():
            arrived(mine, send_small.at[3])

        @pl.when(owner + 1 != seat)
        def _():
            arrived(mine, send_small.at[3])

        for k in range(GRID):
            arrived(other.at[0], send_part.at[0])

    def left_final(n, _):
        arrived(finals.at[0], send_small.at[4])
        return 0

    lax.fori_loop(0, PLANE - 1 + NY * NC - 1, left_final, 0)

    def left_piece(n, _):
        arrived(abuf.at[0, 0], send_piece.at[0])
        return 0

    lax.fori_loop(0, NZ - 1 + 2 * NZ + NZ + 2 * PLANE + PLANE, left_piece, 0)

    def left_weight(n, _):
        arrived(dbuf.at[GRID, 0], send_w.at[0])
        return 0

    lax.fori_loop(0, jnp.where(active, ACTIVE - 1, ACTIVE), left_weight, 0)


def unpack(packed, mean_out, cols_out, errors_out):
    mean_out[...] = packed[8, :]
    cols_out[...] = packed[:GRID, : cols_out.shape[1]]
    errors_out[...] = packed[9, :GRID]


def on_device(activations, weight):
    vmem = pl.BlockSpec(memory_space=pltpu.VMEM)
    dma = pltpu.SemaphoreType.DMA
    f32, bf16 = jnp.float32, jnp.bfloat16
    packed = pl.pallas_call(
        kernel,
        out_shape=jax.ShapeDtypeStruct((16, GROUP), f32),
        in_specs=[vmem, pl.BlockSpec(memory_space=pl.ANY)],
        out_specs=vmem,
        scratch_shapes=[
            pltpu.VMEM((SUB, ROWS // 2, GROUP), bf16),
            pltpu.VMEM((NY, PLANE, ROWS, HALF), bf16),
            pltpu.VMEM((GRID + 1, PLANE, GROUP, WIDE), bf16),
            pltpu.VMEM((GRID + 1, TOKENS, WIDE), f32),
            pltpu.VMEM((GRID, NC, TOKENS, GROUP), f32),
            pltpu.VMEM((GRID, TOKENS, GROUP), f32),
            pltpu.VMEM((PLANE, 8, GROUP), f32),
            pltpu.VMEM((NY, 8, GROUP), f32),
            pltpu.VMEM((NC, 2, 8, GROUP), f32),
            pltpu.VMEM((GROUP, GROUP), f32),
            pltpu.VMEM((GROUP, GROUP), f32),
            pltpu.VMEM((PLANE, GRID - 1, 2, GROUP, GROUP), f32),
            pltpu.VMEM((2, 8, GROUP), f32),
            pltpu.VMEM((8, GROUP), f32),
            pltpu.VMEM((PLANE, 8, GROUP), f32),
            pltpu.VMEM((NY * NC, 8, GROUP), f32),
            dma((5,)),
            dma((1,)),
            dma((1,)),
            dma((1,)),
            dma((SUB,)),
            dma((NZ,)),
            dma((NZ,)),
            dma((NZ,)),
            dma((NZ,)),
            dma((NX * FIRST,)),
            dma((NX * FIRST,)),
            dma((NX * FIRST,)),
            dma((REST,)),
            dma((REST,)),
            dma((REST,)),
            dma((NY * REST,)),
            dma((NY * REST,)),
            dma((NY * REST,)),
            dma((PLANE,)),
            dma((PLANE,)),
            dma((NY,)),
            dma((1,)),
            dma((GRID,)),
            dma((2,)),
            dma((PLANE,)),
            dma((NY * NC,)),
            dma((1,)),
        ],
        compiler_params=pltpu.CompilerParams(
            collective_id=0, has_side_effects=True, vmem_limit_bytes=60 * 1024 * 1024
        ),
    )(activations, weight)
    return pl.pallas_call(
        unpack,
        out_shape=(
            jax.ShapeDtypeStruct((GROUP,), f32),
            jax.ShapeDtypeStruct((GRID, F // (PLANE * NC * NY)), f32),
            jax.ShapeDtypeStruct((GRID,), f32),
        ),
        in_specs=[vmem],
        out_specs=(vmem, vmem, vmem),
    )(packed)


def solution(mesh):
    torus = Mesh(mesh.devices.reshape(NX, NZ, NC, NY), ("x", "z", "c", "y"))
    placed = (P(DP, "y"), P(DP, "y"))
    return jax.shard_map(
        on_device,
        mesh=torus,
        in_specs=placed,
        out_specs=(P(DP), P(None, ("y", "x", "z", "c")), P()),
        check_vma=False,
    )
```

```python
import functools

import jax
import jax.numpy as jnp
from jax import lax
from jax.experimental import pallas as pl
from jax.experimental.pallas import tpu as pltpu
from jax.sharding import Mesh
from jax.sharding import PartitionSpec as P

D = 8192
F = 28672
GROUP = 128
GRID = 4
TOKENS = 768
NX, NZ, NC, NY = 4, 8, 2, 4
PLANE = NX * NZ
ACTIVE = 28
ROWS = 24
HALF = 1024
WIDE = 256
SUB = HALF // GROUP
DP = ("x", "z", "c")
Z_ORDER = (0, -1, 1, -2, 2, -3, 3, -4)
X_ORDER = ((2, 0), (3, 1))
WAVE = (6.579736255173805, -12.987875283620534, 12.207951996649596, -6.691021837978725, 2.380346767313312, -0.5278301996489366)
FIRST = 6
REST = NZ - FIRST
LATER = (0, 1, 3, 6, 9, 12, 16)
MESH_ID = pl.DeviceIdType.MESH


def kernel(
    act, w, out,
    swap, abuf, dbuf, acc, part, other, stat, staty, ends, table, inverse, spread, tiles, mine, finals, finaly,
    send_small, send_piece, send_w, send_part,
    swap_sem, z_sem, xl_sem, xr_sem, x2_sem, yd_sem, yu_sem, y2_sem, qd_sem, qu_sem, q2_sem, ql_sem, qr_sem, qf_sem, w_sem, stat_sem, staty_sem, ends_sem,
    part_sem, tile_sem, fin_sem, finy_sem, own_sem,
):
    x, z, c, y = (lax.axis_index(name) for name in ("x", "z", "c", "y"))
    me = x * NZ + z
    def works(chip):
        return lax.rem(chip, 10) != 1

    def pair_of(chip):
        return chip - (chip + 8) // 10

    active = works(me)

    def device(dx=0, dz=0, dc=0, dy=0):
        return {
            "x": lax.rem(x + dx + NX, NX),
            "z": lax.rem(z + dz + NZ, NZ),
            "c": lax.rem(c + dc, NC),
            "y": lax.rem(y + dy + NY, NY),
        }

    def remote(src, dst, send, recv, to):
        return pltpu.make_async_remote_copy(
            src_ref=src, dst_ref=dst, send_sem=send, recv_sem=recv, device_id=to, device_id_type=MESH_ID
        )

    def arrived(ref, sem):
        pltpu.make_async_copy(ref, ref, sem).wait()

    barrier = pltpu.get_barrier_semaphore()

    def greet(n, _):
        to = device(n // (NZ * NC), lax.rem(n // NC, NZ), lax.rem(n, NC))
        pl.semaphore_signal(barrier, inc=1, device_id=to, device_id_type=MESH_ID)
        return 0

    lax.fori_loop(1, PLANE * NC, greet, 0)
    for dy in range(1, NY):
        for dc in range(NC):
            pl.semaphore_signal(barrier, inc=1, device_id=device(dy=dy, dc=dc), device_id_type=MESH_ID)
    for k in range(GRID + 1):
        acc[k] = jnp.zeros((TOKENS, WIDE), jnp.float32)
    pl.semaphore_wait(barrier, PLANE * NC - 1 + (NY - 1) * NC)

    def lanes(group):
        return pl.ds(pl.multiple_of(group * GROUP, GROUP), GROUP)

    for j in range(SUB):
        remote(
            act.at[:, lanes(2 * j + 1 - c)], swap.at[j], send_small.at[0], swap_sem.at[j], device(dc=1)
        ).start()
    here = c == 0
    out[...] = jnp.zeros((16, GROUP), jnp.float32)
    for j in range(SUB):
        arrived(swap.at[j], swap_sem.at[j])
        own = act[:, lanes(2 * j + c)].astype(jnp.float32)
        peer = swap[j].astype(jnp.float32)
        block = jnp.concatenate([jnp.where(here, own, peer), jnp.where(here, peer, own)], axis=0)
        stat[me, j : j + 1, :] = jnp.sum(jnp.abs(block), axis=0, keepdims=True)
        abuf[y, me, :, j * GROUP : (j + 1) * GROUP] = block.astype(jnp.bfloat16)

    def send_stat(n, _):
        to = device(n // NZ, lax.rem(n, NZ))
        remote(stat.at[me], stat.at[me], send_small.at[1], stat_sem.at[me], to).start()
        return 0

    lax.fori_loop(1, PLANE, send_stat, 0)

    def columns_of(pair):
        return w.at[:, pl.ds(pl.multiple_of(pair * WIDE, WIDE), WIDE)]

    def index_of(to):
        return to["x"] * NZ + to["z"]

    def send_weight(dx, dz):
        to = device(dx, dz)
        there = index_of(to)

        @pl.when(works(there))
        def _():
            columns = columns_of(pair_of(there))
            if dx == 0 and dz == 0:
                pltpu.make_async_copy(columns, dbuf.at[GRID, me], own_sem.at[0]).start()
            else:
                remote(columns, dbuf.at[GRID, me], send_w.at[0], w_sem.at[me], to).start()

    def along(index):
        return lax.rem(z + index + NZ, NZ)

    def piece(yy, xx, k):
        return abuf.at[lax.rem(yy + NY, NY), lax.rem(xx + NX, NX) * NZ + along(Z_ORDER[k])]

    def pass_on(ref, sem, **to):
        remote(ref, ref, send_piece.at[0], sem, device(**to)).start()

    def up_and_down(ref, n):
        pass_on(ref, yd_sem.at[n], dy=1)
        pass_on(ref, yu_sem.at[n], dy=-1)

    def hear_stat(n, _):
        there = lax.rem(x + n // NZ, NX) * NZ + lax.rem(z + lax.rem(n, NZ), NZ)
        arrived(stat.at[there], stat_sem.at[there])
        return 0

    def left_and_right(ref, m):
        pass_on(ref, ql_sem.at[m], dx=1)
        pass_on(ref, qr_sem.at[m], dx=-1)

    for k in range(NZ):
        ref = piece(y, x, k)
        if k == 0:
            for n in range(1, NZ):
                pass_on(ref, z_sem.at[n], dz=-Z_ORDER[n])
        else:
            arrived(ref, z_sem.at[k])
        if k < FIRST:
            pass_on(ref, xl_sem.at[k], dx=1)
            pass_on(ref, xr_sem.at[k], dx=-1)
            up_and_down(ref, k)
        else:
            pass_on(ref, qd_sem.at[k - FIRST], dy=1)
            pass_on(ref, qu_sem.at[k - FIRST], dy=-1)
            left_and_right(ref, k - FIRST)
        for dx in X_ORDER[0]:
            send_weight(dx, Z_ORDER[7 - k])
        if k == 2:
            lax.fori_loop(1, PLANE, hear_stat, 0)
            staty[y] = jnp.sum(stat[...], axis=0)
            for dy in range(1, NY):
                remote(staty.at[y], staty.at[y], send_small.at[1], staty_sem.at[y], device(dy=dy)).start()

    for k in range(FIRST):
        left, right = piece(y, x - 1, k), piece(y, x + 1, k)
        arrived(left, xl_sem.at[k])
        if k < FIRST // 2:
            pass_on(left, x2_sem.at[k], dx=1)
        up_and_down(left, FIRST + 2 * k)
        arrived(right, xr_sem.at[k])
        if k >= FIRST // 2:
            pass_on(right, x2_sem.at[k], dx=-1)
        up_and_down(right, FIRST + 1 + 2 * k)
    for q in range(REST):
        below, above = piece(y - 1, x, FIRST + q), piece(y + 1, x, FIRST + q)
        arrived(below, qd_sem.at[q])
        if q < REST // 2:
            pass_on(below, q2_sem.at[q], dy=1)
        left_and_right(below, REST + 2 * q)
        arrived(above, qu_sem.at[q])
        if q >= REST // 2:
            pass_on(above, q2_sem.at[q], dy=-1)
        left_and_right(above, REST + 1 + 2 * q)

    for dy in range(1, NY):
        there = lax.rem(y + dy, NY)
        arrived(staty.at[there], staty_sem.at[there])
    channel_mean = staty[...].reshape(PLANE, GROUP) / TOKENS + 1e-06
    own_mean = staty[x, pl.ds(z, 1), :] / TOKENS + 1e-06
    out[8:9, :] = own_mean
    log_mean = jnp.log(channel_mean)
    ends[c, 0] = jnp.broadcast_to(jnp.max(log_mean, axis=0, keepdims=True), (8, GROUP))
    ends[c, 1] = jnp.broadcast_to(jnp.min(log_mean, axis=0, keepdims=True), (8, GROUP))
    remote(ends.at[c], ends.at[c], send_small.at[2], ends_sem.at[0], device(dc=1)).start()
    arrived(ends.at[1 - c], ends_sem.at[0])
    top = jnp.max(jnp.maximum(ends[0, 0], ends[1, 0]), axis=(0, 1), keepdims=True)
    bottom = jnp.min(jnp.minimum(ends[0, 1], ends[1, 1]), axis=(0, 1), keepdims=True)
    rows = []
    for k in range(1, GRID):
        ratio = k / GRID
        level = jnp.sqrt(jnp.exp(ratio * top) * jnp.exp(ratio * bottom))
        rows.append(jnp.exp(ratio * log_mean) / level)
    rows.append(jnp.ones((PLANE, GROUP), jnp.float32))
    stacked = jnp.concatenate(rows, axis=0)
    table[...] = stacked.T
    inverse[...] = (1.0 / stacked).T


    def widen(slot):
        factors = pltpu.roll(table[...], GROUP - slot, 1)
        backs = pltpu.roll(inverse[...], GROUP - slot, 1)
        for k in range(GRID - 1):
            at = k * PLANE
            spread[slot, k, 0] = jnp.broadcast_to(factors[:, at : at + 1], (GROUP, GROUP))
            spread[slot, k, 1] = jnp.broadcast_to(backs[:, at : at + 1], (GROUP, GROUP))

    def quantize(slot):
        for half in range(WIDE // GROUP):
            at = slice(half * GROUP, (half + 1) * GROUP)
            weight = dbuf[GRID, slot, :, at].astype(jnp.float32)
            for k in range(GRID):
                scaled = weight if k == 0 else weight * spread[slot, k - 1, 0]
                step = (jnp.max(jnp.abs(scaled), axis=0, keepdims=True) + 1e-06) * (1.0 / 7.0)
                value = scaled * (1.0 / step)
                whole = jnp.round(value)
                rest = value - whole
                square = rest * rest
                wave = jnp.full_like(square, WAVE[-1])
                for term in WAVE[-2::-1]:
                    wave = wave * square + term
                level = whole + rest * square * wave
                result = level * step
                if k > 0:
                    result = result * spread[slot, k - 1, 1]
                dbuf[k, slot, :, at] = result.astype(jnp.bfloat16)

    def slot_of(n):
        n = jnp.int32(n)
        order = jnp.where(n < FIRST, n, jnp.where(n < 3 * FIRST, (n - FIRST) // 2, n - 3 * FIRST))
        beside = jnp.where(lax.rem(n - FIRST + NX * NZ, 2) == 0, -1, 1)
        dx = jnp.where(n < FIRST, 0, jnp.where(n < 3 * FIRST, beside, 2))
        dz = jnp.where(lax.rem(order, 2) == 1, -((order + 1) // 2), order // 2)
        return lax.rem(x + dx + NX, NX) * NZ + lax.rem(z + dz + NZ, NZ)

    def relay(n):
        n = jnp.int32(n)
        slot = slot_of(n)
        below = abuf.at[lax.rem(y + NY - 1, NY), slot]
        above = abuf.at[lax.rem(y + 1, NY), slot]
        arrived(below, yd_sem.at[n])

        @pl.when(lax.rem(n, 2) == 0)
        def _():
            pass_on(below, y2_sem.at[n], dy=1)

        arrived(above, yu_sem.at[n])

        @pl.when(lax.rem(n, 2) == 1)
        def _():
            pass_on(above, y2_sem.at[n], dy=-1)

    def source(i):
        i = jnp.int32(i)
        first, even = i < 2 * NZ, lax.rem(i, 2) == 0
        order = NZ - 1 - lax.rem(i // 2, NZ)
        dx = jnp.where(first, jnp.where(even, X_ORDER[0][0], X_ORDER[0][1]), jnp.where(even, X_ORDER[1][0], X_ORDER[1][1]))
        dz = jnp.where(lax.rem(order, 2) == 1, -((order + 1) // 2), order // 2)
        return lax.rem(x - dx + NX, NX) * NZ + lax.rem(z - dz + NZ, NZ)

    def take(i, wide=True):
        slot = source(i)

        @pl.when(active)
        def _():
            if wide:
                widen(slot)

            @pl.when(slot == me)
            def _():
                pltpu.make_async_copy(dbuf.at[GRID, slot], dbuf.at[GRID, slot], own_sem.at[0]).wait()

            @pl.when(slot != me)
            def _():
                arrived(dbuf.at[GRID, slot], w_sem.at[slot])

            quantize(slot)

    def last(n, _):
        arrived(abuf.at[lax.rem(y + 2, NY), slot_of(n)], y2_sem.at[n])
        return 0

    def multiply(block, k):
        lhs = abuf[block].reshape(TOKENS, HALF)
        rhs = dbuf[k, pl.ds(block * SUB, SUB)].reshape(HALF, WIDE)
        return jnp.dot(lhs, rhs, preferred_element_type=jnp.float32)

    def accumulate(block):
        for k in range(GRID + 1):
            acc[k] += multiply(block, k)

    later = [(dx, Z_ORDER[7 - k]) for k in range(NZ) for dx in X_ORDER[1]]
    for k in range(FIRST):
        far = piece(y, x + 2, k)
        arrived(far, x2_sem.at[k])
        up_and_down(far, 3 * FIRST + k)
        for n in range(3 * k, 3 * k + 3):
            relay(n)
        for item in later[LATER[k] : LATER[k + 1]]:
            send_weight(*item)
        take(k)
    for q in range(REST):
        across = piece(y + 2, x, FIRST + q)
        arrived(across, q2_sem.at[q])
        left_and_right(across, 3 * REST + q)
        take(FIRST + q)

    def side(m, dx):
        q = m if m < REST else (m - REST) // 2 if m < 3 * REST else m - 3 * REST
        dy = 0 if m < REST else (1 if (m - REST) % 2 else -1) if m < 3 * REST else 2
        return piece(y + dy, x + dx, FIRST + q)

    def beside(m):
        arrived(side(m, -1), ql_sem.at[m])
        if m % 2 == 0:
            pass_on(side(m, -1), qf_sem.at[m], dx=1)
        arrived(side(m, 1), qr_sem.at[m])
        if m % 2 == 1:
            pass_on(side(m, 1), qf_sem.at[m], dx=-1)

    for m in range(2 * REST):
        beside(m)

    def two(j, _):
        relay(3 * FIRST + j)

        @pl.when(active)
        def _():
            def ahead(n, _):
                widen(source(n))
                return 0

            lax.fori_loop(2 * NZ + 3 * j, jnp.minimum(2 * NZ + 3 * j + 3, 4 * NZ), ahead, 0)

        take(NZ + j)
        return 0

    def one(i, _):
        take(i, False)
        return 0

    lax.fori_loop(0, FIRST // 2, two, 0)
    for m in range(2 * REST, 3 * REST):
        beside(m)
    lax.fori_loop(FIRST // 2, FIRST, two, 0)
    for m in range(3 * REST, 4 * REST):
        beside(m)
    for i in range(NZ + FIRST, 2 * NZ):
        take(i)
    for m in range(3 * REST):
        arrived(side(m, 2), qf_sem.at[m])
    opposite = lax.rem(x - y + NX, NX) == 2
    sooner = lax.rem(jnp.where(opposite, x + 2, x), NX)
    later_one = lax.rem(jnp.where(opposite, x, x + 2), NX)

    @pl.when(active)
    def _():
        accumulate(sooner)

    lax.fori_loop(2 * NZ, 3 * NZ + 4, one, 0)
    lax.fori_loop(0, NX * FIRST, last, 0)
    for m in range(3 * REST, 4 * REST):
        arrived(side(m, 2), qf_sem.at[m])

    @pl.when(active)
    def _():
        accumulate(later_one)

    lax.fori_loop(3 * NZ + 4, 4 * NZ, one, 0)
    final = lax.rem(x + NX - 1, NX)

    @pl.when(active)
    def _():
        accumulate(lax.rem(x + 1, NX))
        acc[GRID] += multiply(final, GRID)
        for k in range(GRID):
            residue = acc[k] + multiply(final, k) - acc[GRID]
            part[k, 0] = residue[:, :GROUP]
            part[k, 1] = residue[:, GROUP:]
            remote(part.at[k, 1 - c], other.at[k], send_part.at[0], part_sem.at[k], device(dc=1)).start()
        sums = []
        for k in range(GRID):
            arrived(other.at[k], part_sem.at[k])
            residue = part[k, c] + other[k]
            sums.append(jnp.sum(residue * residue, axis=0, keepdims=True))
        mine[...] = jnp.concatenate(sums + [jnp.zeros((GRID, GROUP), jnp.float32)], axis=0)

    @pl.when(jnp.logical_not(active))
    def _():
        mine[...] = jnp.zeros((8, GROUP), jnp.float32)

    seat = 2 * me + c
    tile = 2 * pair_of(me) + c
    owner = (tile // 7) * 8 + lax.rem(tile, 7)

    def send_tile(to_index, slot):
        to = {"x": to_index // (NZ * NC), "z": lax.rem(to_index // NC, NZ), "c": lax.rem(to_index, NC), "y": y}
        same = to_index == seat

        @pl.when(jnp.logical_not(same))
        def _():
            remote(mine, tiles.at[slot], send_small.at[3], tile_sem.at[slot], to).start()

        @pl.when(same)
        def _():
            tiles[slot] = mine[...]

    @pl.when(active)
    def _():
        send_tile(owner, 1)
        send_tile(owner + 1, 0)

    finals[me] = mine[...]

    def send_final(n, _):
        remote(finals.at[me], finals.at[me], send_small.at[4], fin_sem.at[me], device(n // NZ, lax.rem(n, NZ))).start()
        return 0

    lax.fori_loop(1, PLANE, send_final, 0)

    place = lax.rem(seat, 8)
    before = (seat // 8) * 7 + place - 1
    after = before + 1

    def from_other(source):
        return jnp.logical_not(jnp.logical_and(active, source == tile))

    @pl.when(jnp.logical_and(place > 0, from_other(before)))
    def _():
        arrived(tiles.at[0], tile_sem.at[0])

    @pl.when(place == 0)
    def _():
        tiles[0] = jnp.zeros((8, GROUP), jnp.float32)

    @pl.when(jnp.logical_and(place < 7, from_other(after)))
    def _():
        arrived(tiles.at[1], tile_sem.at[1])

    @pl.when(place == 7)
    def _():
        tiles[1] = jnp.zeros((8, GROUP), jnp.float32)

    shift = 16 * place
    lane = lax.broadcasted_iota(jnp.int32, (8, GROUP), 1)
    joined = jnp.where(lane < shift, pltpu.roll(tiles[0], shift, 1), pltpu.roll(tiles[1], shift, 1))
    out[0:8, :] = joined / TOKENS

    def hear_final(n, _):
        there = lax.rem(x + n // NZ, NX) * NZ + lax.rem(z + lax.rem(n, NZ), NZ)
        arrived(finals.at[there], fin_sem.at[there])
        return 0

    lax.fori_loop(1, PLANE, hear_final, 0)
    place_yc = 2 * y + c
    finaly[place_yc] = jnp.sum(finals[...], axis=0)
    for n in range(1, NY * NC):
        to = device(dy=n // NC, dc=n % NC)
        remote(finaly.at[place_yc], finaly.at[place_yc], send_small.at[4], finy_sem.at[place_yc], to).start()
    for n in range(1, NY * NC):
        there = 2 * lax.rem(y + n // NC, NY) + lax.rem(c + n % NC, NC)
        arrived(finaly.at[there], finy_sem.at[there])
    total = jnp.sum(jnp.sum(finaly[...], axis=0), axis=1, keepdims=True)
    row = lax.broadcasted_iota(jnp.int32, (8, GROUP), 0)
    placed = jnp.where(row == lane, jnp.broadcast_to(total / (TOKENS * F), (8, GROUP)), 0.0)
    out[9:10, :] = jnp.sum(placed, axis=0, keepdims=True)

    for j in range(SUB):
        arrived(swap.at[j], send_small.at[0])

    def left_stat(n, _):
        arrived(stat.at[0], send_small.at[1])
        return 0

    lax.fori_loop(0, PLANE - 1 + NY - 1, left_stat, 0)
    arrived(ends.at[0], send_small.at[2])

    @pl.when(active)
    def _():
        @pl.when(owner != seat)
        def _():
            arrived(mine, send_small.at[3])

        @pl.when(owner + 1 != seat)
        def _():
            arrived(mine, send_small.at[3])

        for k in range(GRID):
            arrived(other.at[0], send_part.at[0])

    def left_final(n, _):
        arrived(finals.at[0], send_small.at[4])
        return 0

    lax.fori_loop(0, PLANE - 1 + NY * NC - 1, left_final, 0)

    def left_piece(n, _):
        arrived(abuf.at[0, 0], send_piece.at[0])
        return 0

    lax.fori_loop(0, NZ - 1 + 2 * NZ + NZ + 2 * PLANE + PLANE, left_piece, 0)

    def left_weight(n, _):
        arrived(dbuf.at[GRID, 0], send_w.at[0])
        return 0

    lax.fori_loop(0, jnp.where(active, ACTIVE - 1, ACTIVE), left_weight, 0)


def unpack(packed, mean_out, cols_out, errors_out):
    mean_out[...] = packed[8, :]
    cols_out[...] = packed[:GRID, : cols_out.shape[1]]
    errors_out[...] = packed[9, :GRID]


def on_device(activations, weight):
    vmem = pl.BlockSpec(memory_space=pltpu.VMEM)
    dma = pltpu.SemaphoreType.DMA
    f32, bf16 = jnp.float32, jnp.bfloat16
    packed = pl.pallas_call(
        kernel,
        out_shape=jax.ShapeDtypeStruct((16, GROUP), f32),
        in_specs=[vmem, pl.BlockSpec(memory_space=pl.ANY)],
        out_specs=vmem,
        scratch_shapes=[
            pltpu.VMEM((SUB, ROWS // 2, GROUP), bf16),
            pltpu.VMEM((NY, PLANE, ROWS, HALF), bf16),
            pltpu.VMEM((GRID + 1, PLANE, GROUP, WIDE), bf16),
            pltpu.VMEM((GRID + 1, TOKENS, WIDE), f32),
            pltpu.VMEM((GRID, NC, TOKENS, GROUP), f32),
            pltpu.VMEM((GRID, TOKENS, GROUP), f32),
            pltpu.VMEM((PLANE, 8, GROUP), f32),
            pltpu.VMEM((NY, 8, GROUP), f32),
            pltpu.VMEM((NC, 2, 8, GROUP), f32),
            pltpu.VMEM((GROUP, GROUP), f32),
            pltpu.VMEM((GROUP, GROUP), f32),
            pltpu.VMEM((PLANE, GRID - 1, 2, GROUP, GROUP), f32),
            pltpu.VMEM((2, 8, GROUP), f32),
            pltpu.VMEM((8, GROUP), f32),
            pltpu.VMEM((PLANE, 8, GROUP), f32),
            pltpu.VMEM((NY * NC, 8, GROUP), f32),
            dma((5,)),
            dma((1,)),
            dma((1,)),
            dma((1,)),
            dma((SUB,)),
            dma((NZ,)),
            dma((NZ,)),
            dma((NZ,)),
            dma((NZ,)),
            dma((NX * FIRST,)),
            dma((NX * FIRST,)),
            dma((NX * FIRST,)),
            dma((REST,)),
            dma((REST,)),
            dma((REST,)),
            dma((NY * REST,)),
            dma((NY * REST,)),
            dma((NY * REST,)),
            dma((PLANE,)),
            dma((PLANE,)),
            dma((NY,)),
            dma((1,)),
            dma((GRID,)),
            dma((2,)),
            dma((PLANE,)),
            dma((NY * NC,)),
            dma((1,)),
        ],
        compiler_params=pltpu.CompilerParams(
            collective_id=0, has_side_effects=True, vmem_limit_bytes=60 * 1024 * 1024
        ),
    )(activations, weight)
    return pl.pallas_call(
        unpack,
        out_shape=(
            jax.ShapeDtypeStruct((GROUP,), f32),
            jax.ShapeDtypeStruct((GRID, F // (PLANE * NC * NY)), f32),
            jax.ShapeDtypeStruct((GRID,), f32),
        ),
        in_specs=[vmem],
        out_specs=(vmem, vmem, vmem),
    )(packed)


def solution(mesh):
    torus = Mesh(mesh.devices.reshape(NX, NZ, NC, NY), ("x", "z", "c", "y"))
    placed = (P(DP, "y"), P(DP, "y"))
    return jax.shard_map(
        on_device,
        mesh=torus,
        in_specs=placed,
        out_specs=(P(DP), P(None, ("y", "x", "z", "c")), P()),
        check_vma=False,
    )
```
